512 devices in a mesh: tm: 32 (over x_hi, y, core), space: 16 (over x_lo, z).
Axes of the slice: x: 4 (x_hi: 2, x_lo: 2; x = x_hi * 2 + x_lo), y: 8, z: 8, core: 2. Of those that a mesh axis runs over, the one named last changes fastest.
Arguments:
- increments: float32 [64, 1024, 2048], P('tm', 'space'), may hold values from -6 to 6
- precision: float32 [64, 1024, 2048], P('tm', 'space'), may hold values from 0.5 to 4
- courant_rows: float32 [1024, 2048], P('space'), may hold values from 0.05 to 0.45
- courant_cols: float32 [1024, 2048], P('space'), may hold values from 0.05 to 0.45
- wind_codes: int32 [64, 128, 16], P('tm', 'space'), may hold values from 0 to 3
Outputs:
- misfit: float32 [64, 1024, 2048], P('tm', 'space')
- adjoint_image: float32 [64, 1024, 2048], P('tm', 'space')
The draws below stay inside these ranges and needn't reach their ends.
All inputs are finite; a program needn't handle non-finite values.
Results may differ from the reference program's by a relative error of at most 0.00002.
Values sent between devices are 32-bit elements; how exact they have to be, the bound alone decides.
No kernel may reach another device: no remote copies, remote signals or barrier semaphores. Data moves between devices by JAX's collectives and lax.ppermute only.
A program may use at most 64 MiB of HBM per device.

```python
import math
import jax
import jax.numpy as jnp

NY = 2048
BX = 8
BY = 128
SWEEPS = 2
STEPS = 64
NX = 1024


def with_ends(array, rng, smallest, largest):
    longest = array.shape.index(max(array.shape))
    spots = []
    for shift in (0, 1):
        where = [jax.random.randint(jax.random.fold_in(rng, axis), (), 0, length) for axis, length in enumerate(array.shape)]
        where[longest] = (where[longest] + shift) % array.shape[longest]
        spots.append(tuple(where))
    return array.at[spots[0]].set(smallest).at[spots[1]].set(largest)


def levels(key, extent, cuts, low, high):
    factor_of = 1.0
    for axis_at, shards_of in cuts:
        draws = jax.random.uniform(jax.random.fold_in(jax.random.fold_in(key, 6), axis_at), (shards_of,), jnp.float32, low / len(cuts), high / len(cuts))
        factor_of = factor_of * jnp.repeat(jnp.exp(draws), extent[axis_at] // shards_of).reshape((-1,) + (1,) * (len(extent) - 1 - axis_at))
    return factor_of


def centred(key, extent, scale, most, cuts=(), dtype=jnp.bfloat16):
    drawn = scale * jax.random.normal(key, extent, jnp.float32)
    if cuts:
        drawn = drawn * levels(key, extent, cuts, -0.22, 0.18)
    return jnp.clip(drawn, -most, most).astype(dtype)


def setup_inputs(seed: int = 0) -> dict:
    key_of = jax.random.split(jax.random.key(seed), 6)
    return {
        "increments": centred(key_of[0], (STEPS, NX, NY), 1.0, 6.0, ((0, 32), (1, 16)), jnp.float32),
        "precision": jnp.clip(jnp.exp(math.log(4.0) - 2.0794415 * jax.random.uniform(key_of[1], (STEPS, NX, NY), jnp.float32) ** levels(key_of[1], (STEPS, NX, NY), ((0, 32), (1, 16)), -0.2, 0.2)), 0.5, 4.0),
        "courant_rows": jnp.clip(0.05 + 0.39999999 * jax.random.uniform(key_of[2], (NX, NY), jnp.float32) ** levels(key_of[2], (NX, NY), ((0, 16),), -0.2, 0.2), 0.05, 0.45),
        "courant_cols": jnp.clip(0.05 + 0.39999999 * jax.random.uniform(key_of[3], (NX, NY), jnp.float32) ** levels(key_of[3], (NX, NY), ((0, 16),), -0.2, 0.2), 0.05, 0.45),
        "wind_codes": with_ends(jax.random.randint(key_of[4], (STEPS, NX // BX, NY // BY), 0, 4), jax.random.fold_in(key_of[4], 1), 0, 3).astype(jnp.int32),
    }


def directions(wind_codes):
    per_cell = jnp.repeat(jnp.repeat(wind_codes, BX, axis=1), BY, axis=2)
    side_rows = 1 - 2 * (per_cell % 2)
    side_cols = 1 - 2 * (per_cell // 2)
    return side_rows, side_cols


def advance(values_in, padded, side_rows, side_cols, courant_rows, courant_cols):
    from_rows = jnp.where(side_rows > 0, padded[:, :-2], padded[:, 2:])
    from_cols = jnp.where(side_cols > 0, jnp.roll(values_in, 1, axis=2), jnp.roll(values_in, -1, axis=2))
    return (1.0 - courant_rows - courant_cols) * values_in + courant_rows * from_rows + courant_cols * from_cols


def smooth(values_in):
    field = values_in
    for sweep in range(SWEEPS):
        padded = jnp.pad(field, ((0, 0), (1, 1), (0, 0)))
        beside_all = padded[:, :-2] + padded[:, 2:] + jnp.roll(field, 1, axis=2) + jnp.roll(field, -1, axis=2)
        field = field + 0.2 * (beside_all - 4.0 * field)
    return field


def adjoint_pieces(values_in, side_rows, courant_rows):
    along_rows = courant_rows * values_in
    return jnp.stack([jnp.where(side_rows > 0, along_rows, 0.0), jnp.where(side_rows < 0, along_rows, 0.0)], axis=1)


def retreat(values_in, padded_pieces, side_rows, side_cols, courant_rows, courant_cols):
    from_rows = padded_pieces[:, 0, 2:] + padded_pieces[:, 1, :-2]
    along_cols = courant_cols * values_in
    plus_cols = jnp.where(side_cols > 0, along_cols, 0.0)
    minus_cols = jnp.where(side_cols < 0, along_cols, 0.0)
    from_cols = jnp.roll(plus_cols, -1, axis=2) + jnp.roll(minus_cols, 1, axis=2)
    return (1.0 - courant_rows - courant_cols) * values_in + from_rows + from_cols


def reference(increments, precision, courant_rows, courant_cols, wind_codes):
    side_rows, side_cols = directions(wind_codes)
    shifted = jnp.concatenate([jnp.zeros_like(increments[:1]), increments[:-1]], axis=0)
    padded = jnp.pad(shifted, ((0, 0), (1, 1), (0, 0)))
    moved = advance(shifted, padded, side_rows, side_cols, courant_rows, courant_cols)
    misfit = increments - moved
    weighted = smooth(precision * smooth(misfit))
    pieces = adjoint_pieces(weighted, side_rows, courant_rows)
    padded_pieces = jnp.pad(pieces, ((0, 0), (0, 0), (1, 1), (0, 0)))
    images = retreat(weighted, padded_pieces, side_rows, side_cols, courant_rows, courant_cols)
    following = jnp.concatenate([images[1:], jnp.zeros_like(images[:1])], axis=0)
    adjoint_image = weighted - following
    return misfit, adjoint_image
```

```python
import jax
import jax.numpy as jnp
from jax import lax
from jax.experimental import pallas as pl
from jax.experimental.pallas import tpu as pltpu
from jax.sharding import PartitionSpec as P

F = 10
NJ = 16
G = 8
L = 128
C4 = 0.04 * 0.04
VMEM = pltpu.VMEM


def lanes():
    return lax.broadcasted_iota(jnp.int32, (1, 8, L), 2)


def sublanes(shape):
    return lax.broadcasted_iota(jnp.int32, shape, len(shape) - 2)


def load(nat, f, j0):
    return jnp.stack([nat[j0 + g, pl.ds(f, 8, stride=F), :] for g in range(G)])


def save(nat, f, j0, x):
    for g in range(G):
        nat[j0 + g, pl.ds(f, 8, stride=F), :] = x[g]


def put(t, f, j0, x):
    t[f + 1, j0 + 1 : j0 + 1 + G] = x
    if j0 == 0:
        t[f + 1, NJ + 1] = x[0]
    if j0 + G == NJ:
        t[f + 1, 0] = x[G - 1]
    if f == F - 1:
        t[0, j0 + 1 : j0 + 1 + G] = pltpu.roll(x, 1, 1)
    if f == 0:
        t[F + 1, j0 + 1 : j0 + 1 + G] = pltpu.roll(x, 7, 1)


def beside(u):
    first = lanes() == 0
    last = lanes() == L - 1
    right_of = pltpu.roll(u[: G + 1], 1, 2)
    left_of = pltpu.roll(u[1:], L - 1, 2)
    left = jnp.where(first, right_of[:G], right_of[1:])
    right = jnp.where(last, left_of[1:], left_of[:G])
    return left, right


def chunks():
    return [(f, j0) for f in range(F) for j0 in range(0, NJ, G)]


def weights(wn, f, j0):
    return load(wn[0], f, j0), load(wn[1], f, j0)


def masks(code):
    mc = code < 1.5
    mr = jnp.where(mc, code, code - 2.0) < 0.5
    return mr, mc


def to_t(nat, t):
    for f, j0 in chunks():
        put(t, f, j0, load(nat, f, j0))


def misfit_stage(tu, vn, code, wn, tout, out):
    for f, j0 in chunks():
        u = tu[f + 1, j0 : j0 + G + 2]
        left, right = beside(u)
        up = tu[f, j0 + 1 : j0 + 1 + G]
        down = tu[f + 2, j0 + 1 : j0 + 1 + G]
        mr, mc = masks(load(code, f, j0))
        cr, cc = weights(wn, f, j0)
        moved = (
            (1.0 - cr - cc) * u[1 : G + 1]
            + cr * jnp.where(mr, up, down)
            + cc * jnp.where(mc, left, right)
        )
        mis = load(vn, f, j0) - moved
        put(tout, f, j0, mis)
        if out is not None:
            save(out, f, j0, mis)


def sweep_stage(tin, tout, after):
    for f, j0 in chunks():
        u = tin[f + 1, j0 : j0 + G + 2]
        left, right = beside(u)
        up = tin[f, j0 + 1 : j0 + 1 + G]
        down = tin[f + 2, j0 + 1 : j0 + 1 + G]
        x = ((up + down) + (left + right)) + u[1 : G + 1]
        put(tout, f, j0, after(x, f, j0))


def smooth_stages(tin, tmp, pn, tout, inside):
    def mask(x, f, j0):
        return jnp.where(inside(f), x, 0.0)

    def scale(x, f, j0):
        return (load(pn, f, j0) * C4) * x

    sweep_stage(tin, tmp, mask)
    sweep_stage(tmp, tin, scale)
    sweep_stage(tin, tmp, mask)
    sweep_stage(tmp, tout, lambda x, f, j0: x)


def adjoint_stage(tw, code, wn, ta, tb, tc):
    first = lanes() == 0
    last = lanes() == L - 1
    for f, j0 in chunks():
        w = tw[f + 1, j0 + 1 : j0 + 1 + G]
        mr, mc = masks(load(code, f, j0))
        cr, cc = weights(wn, f, j0)
        along = cr * w
        lower = jnp.where(mr, along, 0.0)
        put(ta, f, j0, lower)
        put(tb, f, j0, along - lower)
        along = cc * w
        plus = jnp.where(mc, along, 0.0)
        put(tc, f, j0, plus)
        tc2 = along - plus
        put(tw2_ref[0], f, j0, tc2)
        base_ref[0][f, j0 : j0 + G] = (1.0 - cr - cc) * w
    for f, j0 in chunks():
        plus = tc[f + 1, j0 + 1 : j0 + G + 2]
        minus = tw2_ref[0][f + 1, j0 : j0 + G + 1]
        left_of = pltpu.roll(plus, L - 1, 2)
        right_of = pltpu.roll(minus, 1, 2)
        cols = jnp.where(last, left_of[1:], left_of[:G]) + jnp.where(
            first, right_of[:G], right_of[1:]
        )
        rows = ta[f + 2, j0 + 1 : j0 + 1 + G] + tb[f, j0 + 1 : j0 + 1 + G]
        base_ref[0][f, j0 : j0 + G] = base_ref[0][f, j0 : j0 + G] + rows + cols


tw2_ref = [None]
base_ref = [None]


def parity():
    return lax.axis_index("tm") % 2


def code_rows(codes, step):
    c = codes[step].astype(jnp.float32)
    return [jnp.broadcast_to(c[:, j : j + 1], (8, L)) for j in range(NJ)]


def pack_kernel(inc, prec, edge, codes, bulk_o, bulk_e, up, dn, sems):
    even = parity() == 0

    def forward(dst):
        return [pltpu.make_async_copy(inc.at[1], dst.at[pl.ds(0, 64)], sems.at[0])]

    def backward(dst):
        return [
            pltpu.make_async_copy(inc.at[0], dst.at[pl.ds(0, 64)], sems.at[1]),
            pltpu.make_async_copy(prec.at[0], dst.at[pl.ds(64, 64)], sems.at[2]),
        ]

    def start(fwd, bwd):
        for c in forward(fwd) + backward(bwd):
            c.start()

    @pl.when(even)
    def _():
        start(bulk_e, bulk_o)

    @pl.when(jnp.logical_not(even))
    def _():
        start(bulk_o, bulk_e)

    row = sublanes((8, L))
    rows0 = code_rows(codes, 0)
    rows1 = code_rows(codes, 1)
    for j in range(NJ):
        cols = pl.ds(j * L, L)
        bulk_o[128:136, cols] = rows0[j]
        bulk_e[128:136, cols] = rows0[j]
        inc0t, inc0b, inc1t, inc1b, p0t, p0b, p1t, p1b, crt, crb, cct, ccb = [
            edge[k, :, cols] for k in range(12)
        ]
        c0t = jnp.broadcast_to(rows0[j][0:1], (8, L))
        c0b = jnp.broadcast_to(rows0[j][7:8], (8, L))
        c1t = jnp.broadcast_to(rows1[j][0:1], (8, L))
        c1b = jnp.broadcast_to(rows1[j][7:8], (8, L))
        up[0:8, cols] = jnp.where(row < 2, c0b, inc0b)
        up[8:16, cols] = jnp.where(row < 2, c1b, inc1b)
        up[16:24, cols] = jnp.where(row < 3, pltpu.roll(p0b, 3, 0), crb)
        up[24:32, cols] = jnp.where(row < 3, pltpu.roll(p1b, 3, 0), ccb)
        dn[0:8, cols] = jnp.where(row > 5, c0t, inc0t)
        dn[8:16, cols] = jnp.where(row > 5, c1t, inc1t)
        dn[16:24, cols] = jnp.where(row > 4, pltpu.roll(p0t, 5, 0), crt)
        dn[24:32, cols] = jnp.where(row > 4, pltpu.roll(p1t, 5, 0), cct)

    @pl.when(even)
    def _():
        for c in forward(bulk_e) + backward(bulk_o):
            c.wait()

    @pl.when(jnp.logical_not(even))
    def _():
        for c in forward(bulk_o) + backward(bulk_e):
            c.wait()


def pack_body(inc, prec, cr, cc, codes, bulk_o, bulk_e, up, dn, edge, sems, esems):
    top, bottom = pl.ds(0, 8), pl.ds(56, 8)
    srcs = []
    for a in (inc.at[0], inc.at[1], prec.at[0], prec.at[1], cr, cc):
        srcs += [a.at[top], a.at[bottom]]
    copies = [pltpu.make_async_copy(s, edge.at[k], esems.at[k]) for k, s in enumerate(srcs)]
    for c in copies:
        c.start()
    for c in copies:
        c.wait()
    pack_kernel(inc, prec, edge, codes, bulk_o, bulk_e, up, dn, sems)


def pack(inc, prec, cr, cc, codes):
    any_spec = pl.BlockSpec(memory_space=pl.ANY)
    vmem = pl.BlockSpec(memory_space=VMEM)
    f32 = lambda *s: jax.ShapeDtypeStruct(s, jnp.float32)
    return pl.pallas_call(
        pack_body,
        in_specs=[any_spec] * 4 + [vmem],
        out_specs=[vmem] * 4,
        out_shape=[f32(136, 2048), f32(136, 2048), f32(32, 2048), f32(32, 2048)],
        scratch_shapes=[
            VMEM((12, 8, 2048), jnp.float32),
            pltpu.SemaphoreType.DMA((3,)),
            pltpu.SemaphoreType.DMA((12,)),
        ],
        compiler_params=pltpu.CompilerParams(vmem_limit_bytes=12 << 20),
        name="pack",
    )(inc, prec, cr, cc, codes)


def corner_body(up, dn, cor_o, cor_e):
    even = parity() == 0
    row = sublanes((8, 2048))

    def forward(dst):
        dst[0:8, :] = up[8:16, :]
        dst[8:16, :] = dn[8:16, :]
        dst[16:24, :] = up[8:16, :]

    def backward(dst):
        dst[0:8, :] = up[0:8, :]
        dst[8:16, :] = dn[0:8, :]
        dst[16:24, :] = jnp.where(row < 4, up[16:24, :], dn[16:24, :])

    @pl.when(even)
    def _():
        forward(cor_e)
        backward(cor_o)

    @pl.when(jnp.logical_not(even))
    def _():
        forward(cor_o)
        backward(cor_e)


def corner(up, dn):
    vmem = pl.BlockSpec(memory_space=VMEM)
    f32 = lambda *s: jax.ShapeDtypeStruct(s, jnp.float32)
    return pl.pallas_call(
        corner_body,
        in_specs=[vmem] * 2,
        out_specs=[vmem] * 2,
        out_shape=[f32(24, 2048), f32(24, 2048)],
        compiler_params=pltpu.CompilerParams(vmem_limit_bytes=4 << 20),
        name="corner",
    )(up, dn)


def main_body(
    inc, prec, cr, cc, codes, up, dn, bulk_o, bulk_e, cor_o, cor_e, mis, adj,
    n_prev, n_inc0, n_inc1, n_next, n_p0, n_p1, n_pn, n_cr, n_cc, n_c0, n_c1, n_cn,
    n_m0, n_m1, n_a0, n_a1,
    tu, ta, tb, tw1, tx, ty, base1, base2, isem, osem,
):
    even = parity() == 0
    slab = lax.axis_index("space")
    own = [(inc.at[0], n_inc0), (inc.at[1], n_inc1), (prec.at[0], n_p0), (prec.at[1], n_p1), (cr, n_cr), (cc, n_cc)]

    def copies(k):
        src, dst = own[k]
        return [
            pltpu.make_async_copy(
                src.at[:, pl.ds(j * L, L)], dst.at[j, pl.ds(8, 64)], isem.at[k * NJ + j]
            )
            for j in range(NJ)
        ]

    for k in range(6):
        for c in copies(k):
            c.start()

    def blk(ref, r, j):
        return ref[r : r + 8, j * L : (j + 1) * L]

    def spread(dst, j, at, x):
        dst[j, at : at + 8] = jnp.broadcast_to(x, (8, L))

    def halo(dst, j, top, bottom):
        dst[j, 0:8] = top
        dst[j, 72:80] = bottom

    rows0 = code_rows(codes, 0)
    rows1 = code_rows(codes, 1)
    for j in range(NJ):
        for n_c, rows, r in ((n_c0, rows0, 0), (n_c1, rows1, 8)):
            for b in range(8):
                spread(n_c, j, 8 + 8 * b, rows[j][b : b + 1])
            spread(n_c, j, 0, blk(up, r, j)[0:1])
            spread(n_c, j, 72, blk(dn, r, j)[7:8])
        halo(n_inc0, j, blk(up, 0, j), blk(dn, 0, j))
        halo(n_inc1, j, blk(up, 8, j), blk(dn, 8, j))
        halo(n_cr, j, blk(up, 16, j), blk(dn, 16, j))
        halo(n_cc, j, blk(up, 24, j), blk(dn, 24, j))
        halo(n_p0, j, pltpu.roll(blk(up, 16, j), 5, 0), pltpu.roll(blk(dn, 16, j), 3, 0))
        halo(n_p1, j, pltpu.roll(blk(up, 24, j), 5, 0), pltpu.roll(blk(dn, 24, j), 3, 0))

    def previous(bulk, cor):
        for j in range(NJ):
            for b in range(8):
                n_prev[j, 8 + 8 * b : 16 + 8 * b] = blk(bulk, 8 * b, j)
            halo(n_prev, j, blk(cor, 0, j), blk(cor, 8, j))

    def following(bulk, cor):
        for j in range(NJ):
            for b in range(8):
                n_next[j, 8 + 8 * b : 16 + 8 * b] = blk(bulk, 8 * b, j)
                n_pn[j, 8 + 8 * b : 16 + 8 * b] = blk(bulk, 64 + 8 * b, j)
                spread(n_cn, j, 8 + 8 * b, bulk[128 + b : 129 + b, j * L : (j + 1) * L])
            halo(n_next, j, blk(cor, 0, j), blk(cor, 8, j))
            spread(n_cn, j, 0, blk(cor, 0, j)[0:1])
            spread(n_cn, j, 72, blk(cor, 8, j)[7:8])
            halo(n_pn, j, pltpu.roll(blk(cor, 16, j), 5, 0), pltpu.roll(blk(cor, 16, j), 3, 0))

    @pl.when(even)
    def _():
        previous(bulk_o, cor_o)
        following(bulk_e, cor_e)

    @pl.when(jnp.logical_not(even))
    def _():
        previous(bulk_e, cor_e)
        following(bulk_o, cor_o)

    for k in range(6):
        for c in copies(k):
            c.wait()

    sub = sublanes((1, 8, L))
    top_out = (sub == 0) & (slab == 0)
    bottom_out = (sub == 7) & (slab == lax.axis_size("space") - 1)

    def inside(f):
        bad = None
        if f < 8:
            bad = top_out
        if f >= 2:
            bad = bottom_out if bad is None else bad | bottom_out
        return jnp.logical_not(bad)

    outs = []

    def emit(nat, dst, base):
        for j in range(NJ):
            c = pltpu.make_async_copy(
                nat.at[j, pl.ds(8, 64)], dst.at[:, pl.ds(j * L, L)], osem.at[base + j]
            )
            c.start()
            outs.append(c)

    wn = (n_cr, n_cc)
    tw2_ref[0] = ty
    to_t(n_inc0, tu)
    misfit_stage(tu, n_inc1, n_c1, wn, ta, n_m1)
    emit(n_m1, mis.at[1], 0)
    smooth_stages(ta, tb, n_p1, tw1, inside)
    base_ref[0] = base1
    adjoint_stage(tw1, n_c1, wn, ta, tb, tx)
    to_t(n_prev, tu)
    misfit_stage(tu, n_inc0, n_c0, wn, ta, n_m0)
    emit(n_m0, mis.at[0], NJ)
    smooth_stages(ta, tb, n_p0, tx, inside)
    for f, j0 in chunks():
        save(n_a0, f, j0, tx[f + 1, j0 + 1 : j0 + 1 + G] - base1[f, j0 : j0 + G])
    emit(n_a0, adj.at[0], 2 * NJ)
    to_t(n_inc1, tu)
    misfit_stage(tu, n_next, n_cn, wn, ta, None)
    smooth_stages(ta, tb, n_pn, tu, inside)
    base_ref[0] = base2
    adjoint_stage(tu, n_cn, wn, ta, tb, tx)
    for f, j0 in chunks():
        save(n_a1, f, j0, tw1[f + 1, j0 + 1 : j0 + 1 + G] - base2[f, j0 : j0 + G])
    emit(n_a1, adj.at[1], 3 * NJ)
    for c in outs:
        c.wait()


def main(*args):
    any_spec = pl.BlockSpec(memory_space=pl.ANY)
    vmem = pl.BlockSpec(memory_space=VMEM)
    nat = VMEM((NJ, 80, L), jnp.float32)
    t = VMEM((F + 2, NJ + 2, 8, L), jnp.float32)
    base = VMEM((F, NJ, 8, L), jnp.float32)
    out = jax.ShapeDtypeStruct((2, 64, 2048), jnp.float32)
    return pl.pallas_call(
        main_body,
        in_specs=[any_spec] * 4 + [vmem] * 7,
        out_specs=[any_spec] * 2,
        out_shape=[out, out],
        scratch_shapes=[nat] * 16
        + [t] * 6
        + [base] * 2
        + [pltpu.SemaphoreType.DMA((6 * NJ,)), pltpu.SemaphoreType.DMA((4 * NJ,))],
        compiler_params=pltpu.CompilerParams(vmem_limit_bytes=40 << 20),
        name="main",
    )(*args)


def permute(x, rule):
    axes = ("tm", "space")
    nt, ns = lax.axis_size("tm"), lax.axis_size("space")
    pairs = []
    for t in range(nt):
        for s in range(ns):
            a, b = rule(t, s)
            if 0 <= a < nt and 0 <= b < ns:
                pairs.append((t * ns + s, a * ns + b))
    return lax.ppermute(x, axes, pairs)


def off_chip(t, s):
    return (t - 1 if t % 2 == 0 else t + 1), s


def on_chip(t, s):
    return (t + 1 if t % 2 == 0 else t - 1), s


def on_device(inc, prec, cr, cc, codes):
    bulk_o, bulk_e, up, dn = pack(inc, prec, cr, cc, codes)
    bulk_o = permute(bulk_o, off_chip)
    up = permute(up, lambda t, s: (t, s + 1))
    bulk_e = permute(bulk_e, on_chip)
    dn = permute(dn, lambda t, s: (t, s - 1))
    cor_o, cor_e = corner(up, dn)
    cor_e = permute(cor_e, on_chip)
    cor_o = permute(cor_o, off_chip)
    return tuple(main(inc, prec, cr, cc, codes, up, dn, bulk_o, bulk_e, cor_o, cor_e))


def solution(mesh):
    in_specs = (
        P("tm", "space", None),
        P("tm", "space", None),
        P("space", None),
        P("space", None),
        P("tm", "space", None),
    )
    out_specs = (P("tm", "space", None), P("tm", "space", None))
    return jax.shard_map(
        on_device, mesh=mesh, in_specs=in_specs, out_specs=out_specs, check_vma=False
    )
```

```python
import jax
import jax.numpy as jnp
from jax import lax
from jax.experimental import pallas as pl
from jax.experimental.pallas import tpu as pltpu
from jax.sharding import PartitionSpec as P


F = 10
NJ = 16
G = 4
L = 128
C4 = 0.04 * 0.04
VMEM = pltpu.VMEM


def lanes():
    return lax.broadcasted_iota(jnp.int32, (1, 8, L), 2)


def sublanes(shape):
    return lax.broadcasted_iota(jnp.int32, shape, len(shape) - 2)


def load(nat, f, j0, n):
    return jnp.stack([nat[(j0 + g) % NJ, pl.ds(f, 8, stride=F), :] for g in range(n)])


def save(nat, f, j0, x):
    for g in range(G):
        nat[j0 + g, pl.ds(f, 8, stride=F), :] = x[g]


def load_t(t, f, j0, n):
    parts = []
    if j0 < 0:
        parts.append(t[f, NJ - 1 : NJ])
    parts.append(t[f, max(j0, 0) : min(j0 + n, NJ)])
    if j0 + n > NJ:
        parts.append(t[f, 0:1])
    return parts[0] if len(parts) == 1 else jnp.concatenate(parts, axis=0)


def beside(u):
    first = lanes() == 0
    last = lanes() == L - 1
    right_of = pltpu.roll(u[: G + 1], 1, 2)
    left_of = pltpu.roll(u[1:], L - 1, 2)
    left = jnp.where(first, right_of[:G], right_of[1:])
    right = jnp.where(last, left_of[1:], left_of[:G])
    return left, right


def masks(code):
    mc = code < 1.5
    mr = jnp.where(mc, code, code - 2.0) < 0.5
    return mr, mc


def stencil(get, visit):
    for j0 in range(0, NJ, G):
        above = pltpu.roll(get(F - 1, j0, G), 1, 1)
        wide = get(0, j0 - 1, G + 2)
        for f in range(F):
            if f < F - 1:
                after = get(f + 1, j0 - 1, G + 2)
                below = after[1 : G + 1]
            else:
                after = None
                below = pltpu.roll(get(0, j0, G), 7, 1)
            visit(f, j0, wide, above, below)
            above = wide[1 : G + 1]
            wide = after


def misfit_stage(un, vn, code, wn, tout, out):
    def visit(f, j0, u, up, down):
        left, right = beside(u)
        mr, mc = masks(load(code, f, j0, G))
        cr, cc = load(wn[0], f, j0, G), load(wn[1], f, j0, G)
        moved = (
            (1.0 - cr - cc) * u[1 : G + 1]
            + cr * jnp.where(mr, up, down)
            + cc * jnp.where(mc, left, right)
        )
        mis = load(vn, f, j0, G) - moved
        tout[f, j0 : j0 + G] = mis
        if out is not None:
            save(out, f, j0, mis)

    stencil(lambda f, j0, n: load(un, f, j0, n), visit)


def sweep_stage(tin, tout, after):
    def visit(f, j0, u, up, down):
        left, right = beside(u)
        x = ((up + down) + (left + right)) + u[1 : G + 1]
        tout[f, j0 : j0 + G] = after(x, f, j0)

    stencil(lambda f, j0, n: load_t(tin, f, j0, n), visit)


def smooth_stages(tin, tmp, pn, tout, inside):
    def mask(x, f, j0):
        return jnp.where(inside(f), x, 0.0)

    def scale(x, f, j0):
        return (load(pn, f, j0, G) * C4) * x

    sweep_stage(tin, tmp, mask)
    sweep_stage(tmp, tin, scale)
    sweep_stage(tin, tmp, mask)
    sweep_stage(tmp, tout, lambda x, f, j0: x)


def adjoint_stage(tw, code, wn, emit):
    first = lanes() == 0
    last = lanes() == L - 1

    def pieces(f, j0):
        w = load_t(tw, f, j0 - 1, G + 2)
        mr, mc = masks(load(code, f, j0 - 1, G + 2))
        mr = mr[1 : G + 1]
        cr = load(wn[0], f, j0, G)
        cc = load(wn[1], f, j0 - 1, G + 2)
        mid = w[1 : G + 1]
        rows = cr * mid
        lower = jnp.where(mr, rows, 0.0)
        cols = cc * w
        plus = pltpu.roll(jnp.where(mc, cols, 0.0)[1:], L - 1, 2)
        minus = pltpu.roll(jnp.where(mc, 0.0, cols)[: G + 1], 1, 2)
        image = (
            (1.0 - cr - cc[1 : G + 1]) * mid
            + jnp.where(last, plus[1:], plus[:G])
            + jnp.where(first, minus[:G], minus[1:])
        )
        return image, lower, rows - lower

    def upper_only(f, j0):
        mr, _ = masks(load(code, f, j0, G))
        return jnp.where(mr, 0.0, load(wn[0], f, j0, G) * load_t(tw, f, j0, G))

    for j0 in range(0, NJ, G):
        above = pltpu.roll(upper_only(F - 1, j0), 1, 1)
        image, lower, upper = pieces(0, j0)
        lower0 = pltpu.roll(lower, 7, 1)
        for f in range(F):
            if f < F - 1:
                after = pieces(f + 1, j0)
                below = after[1]
            else:
                after = None
                below = lower0
            emit(f, j0, image + (above + below))
            above = upper
            if after is not None:
                image, lower, upper = after


def parity():
    return lax.axis_index("tm") % 2


def code_rows(codes, step):
    c = codes[step].astype(jnp.float32)
    return [jnp.broadcast_to(c[:, j : j + 1], (8, L)) for j in range(NJ)]


def pack_kernel(copies, inc, prec, edge, codes, bulk_o, bulk_e, up, dn, sems):
    even = parity() == 0

    def forward(dst):
        return [pltpu.make_async_copy(inc.at[1], dst.at[pl.ds(0, 64)], sems.at[0])]

    def backward(dst):
        return [
            pltpu.make_async_copy(inc.at[0], dst.at[pl.ds(0, 64)], sems.at[1]),
            pltpu.make_async_copy(prec.at[0], dst.at[pl.ds(64, 64)], sems.at[2]),
        ]

    def start(fwd, bwd):
        for c in forward(fwd) + backward(bwd):
            c.start()

    @pl.when(even)
    def _():
        start(bulk_e, bulk_o)

    @pl.when(jnp.logical_not(even))
    def _():
        start(bulk_o, bulk_e)

    for c in copies:
        c.wait()
    row = sublanes((8, L))
    rows0 = code_rows(codes, 0)
    rows1 = code_rows(codes, 1)
    for j in range(NJ):
        cols = pl.ds(j * L, L)
        bulk_o[128:136, cols] = rows0[j]
        bulk_e[128:136, cols] = rows0[j]
        inc0t, inc0b, inc1t, inc1b, p0t, p0b, p1t, p1b, crt, crb, cct, ccb = [
            edge[k, :, cols] for k in range(12)
        ]
        c0t = jnp.broadcast_to(rows0[j][0:1], (8, L))
        c0b = jnp.broadcast_to(rows0[j][7:8], (8, L))
        c1t = jnp.broadcast_to(rows1[j][0:1], (8, L))
        c1b = jnp.broadcast_to(rows1[j][7:8], (8, L))
        up[0:8, cols] = jnp.where(row < 2, c0b, inc0b)
        up[8:16, cols] = jnp.where(row < 2, c1b, inc1b)
        up[16:24, cols] = jnp.where(row < 3, pltpu.roll(p0b, 3, 0), crb)
        up[24:32, cols] = jnp.where(row < 3, pltpu.roll(p1b, 3, 0), ccb)
        dn[0:8, cols] = jnp.where(row > 5, c0t, inc0t)
        dn[8:16, cols] = jnp.where(row > 5, c1t, inc1t)
        dn[16:24, cols] = jnp.where(row > 4, pltpu.roll(p0t, 5, 0), crt)
        dn[24:32, cols] = jnp.where(row > 4, pltpu.roll(p1t, 5, 0), cct)

    @pl.when(even)
    def _():
        for c in forward(bulk_e) + backward(bulk_o):
            c.wait()

    @pl.when(jnp.logical_not(even))
    def _():
        for c in forward(bulk_o) + backward(bulk_e):
            c.wait()


def pack_body(inc, prec, cr, cc, codes_hbm, bulk_o, bulk_e, up, dn, codes, edge, sems, esems):
    top, bottom = pl.ds(0, 8), pl.ds(56, 8)
    srcs = []
    for a in (inc.at[0], inc.at[1], prec.at[0], prec.at[1], cr, cc):
        srcs += [a.at[top], a.at[bottom]]
    copies = [pltpu.make_async_copy(codes_hbm, codes, esems.at[12])]
    copies += [pltpu.make_async_copy(s, edge.at[k], esems.at[k]) for k, s in enumerate(srcs)]
    for c in copies:
        c.start()
    pack_kernel(copies, inc, prec, edge, codes, bulk_o, bulk_e, up, dn, sems)


def pack(inc, prec, cr, cc, codes):
    any_spec = pl.BlockSpec(memory_space=pltpu.HBM)
    vmem = pl.BlockSpec(memory_space=VMEM)
    f32 = lambda *s: jax.ShapeDtypeStruct(s, jnp.float32)
    return pl.pallas_call(
        pack_body,
        in_specs=[any_spec] * 5,
        out_specs=[vmem] * 4,
        out_shape=[f32(136, 2048), f32(160, 2048), f32(32, 2048), f32(32, 2048)],
        scratch_shapes=[
            VMEM((2, 8, 16), jnp.int32),
            VMEM((12, 8, 2048), jnp.float32),
            pltpu.SemaphoreType.DMA((3,)),
            pltpu.SemaphoreType.DMA((13,)),
        ],
        compiler_params=pltpu.CompilerParams(vmem_limit_bytes=12 << 20),
        name="pack",
    )(*(pltpu.with_memory_space_constraint(a, pltpu.HBM) for a in (inc, prec, cr, cc, codes)))


def corner_body(up, dn, bulk_in, cor_o, bulk_e):
    del bulk_in
    cor_e = bulk_e.at[136:160]
    even = parity() == 0
    row = sublanes((8, 2048))

    def forward(dst):
        dst[0:8, :] = up[8:16, :]
        dst[8:16, :] = dn[8:16, :]
        dst[16:24, :] = up[8:16, :]

    def backward(dst):
        dst[0:8, :] = up[0:8, :]
        dst[8:16, :] = dn[0:8, :]
        dst[16:24, :] = jnp.where(row < 4, up[16:24, :], dn[16:24, :])

    @pl.when(even)
    def _():
        forward(cor_e)
        backward(cor_o)

    @pl.when(jnp.logical_not(even))
    def _():
        forward(cor_o)
        backward(cor_e)


def corner(up, dn, bulk_e):
    vmem = pl.BlockSpec(memory_space=VMEM)
    f32 = lambda *s: jax.ShapeDtypeStruct(s, jnp.float32)
    return pl.pallas_call(
        corner_body,
        in_specs=[vmem] * 2 + [pl.BlockSpec(memory_space=pl.ANY)],
        out_specs=[vmem] * 2,
        out_shape=[f32(24, 2048), f32(160, 2048)],
        input_output_aliases={2: 1},
        compiler_params=pltpu.CompilerParams(vmem_limit_bytes=8 << 20),
        name="corner",
    )(up, dn, bulk_e)


def blk(ref, r, j):
    return ref[r : r + 8, j * L : (j + 1) * L]


def spread(dst, j, at, x):
    dst[j, at : at + 8] = jnp.broadcast_to(x, (8, L))


def halo(dst, j, top, bottom):
    dst[j, 0:8] = top
    dst[j, 72:80] = bottom


def fetch(pairs, sem):
    copies = [
        pltpu.make_async_copy(
            src.at[:, pl.ds(j * L, L)], dst.at[j, pl.ds(8, 64)], sem.at[k * NJ + j]
        )
        for k, (src, dst) in enumerate(pairs)
        for j in range(NJ)
    ]
    for c in copies:
        c.start()
    return copies


def emit_out(nat, dst, sem, base):
    copies = [
        pltpu.make_async_copy(
            nat.at[j, pl.ds(8, 64)], dst.at[:, pl.ds(j * L, L)], sem.at[base + j]
        )
        for j in range(NJ)
    ]
    for c in copies:
        c.start()
    return copies


def inside_rows():
    slab = lax.axis_index("space")
    sub = sublanes((1, 8, L))
    top_out = (sub == 0) & (slab == 0)
    bottom_out = (sub == 7) & (slab == lax.axis_size("space") - 1)

    def inside(f):
        bad = None
        if f < 8:
            bad = top_out
        if f >= 2:
            bad = bottom_out if bad is None else bad | bottom_out
        return jnp.logical_not(bad)

    return inside


def own_codes(codes, step, n_c, up, dn, r):
    rows = code_rows(codes, step)
    for j in range(NJ):
        for b in range(8):
            spread(n_c, j, 8 + 8 * b, rows[j][b : b + 1])
        spread(n_c, j, 0, blk(up, r, j)[0:1])
        spread(n_c, j, 72, blk(dn, r, j)[7:8])


def last_body(
    inc, prec, cr, cc, codes, up, dn, mis, w_out, image_out,
    n_inc0, n_inc1, n_p1, n_cr, n_cc, n_c1, n_m1, ta, tb, tw, isem, osem,
):
    copies = fetch(
        [(inc.at[0], n_inc0), (inc.at[1], n_inc1), (prec.at[1], n_p1), (cr, n_cr), (cc, n_cc)], isem
    )
    own_codes(codes, 1, n_c1, up, dn, 8)
    for j in range(NJ):
        halo(n_inc0, j, blk(up, 0, j), blk(dn, 0, j))
        halo(n_inc1, j, blk(up, 8, j), blk(dn, 8, j))
        halo(n_cr, j, blk(up, 16, j), blk(dn, 16, j))
        halo(n_cc, j, blk(up, 24, j), blk(dn, 24, j))
        halo(n_p1, j, pltpu.roll(blk(up, 24, j), 5, 0), pltpu.roll(blk(dn, 24, j), 3, 0))
    for c in copies:
        c.wait()
    wn = (n_cr, n_cc)
    inside = inside_rows()
    misfit_stage(n_inc0, n_inc1, n_c1, wn, ta, n_m1)
    outs = emit_out(n_m1, mis.at[1], osem, 0)
    smooth_stages(ta, tb, n_p1, tw, inside)

    def emit(f, j0, image):
        image_out[f, j0 : j0 + G] = image
        w_out[f, j0 : j0 + G] = tw[f, j0 : j0 + G]

    adjoint_stage(tw, n_c1, wn, emit)
    for c in outs:
        c.wait()


def first_body(
    inc, prec, cr, cc, codes, up, dn, bulk_o, bulk_e, cor_o, w1, image1, mis_in,
    mis, adj,
    n_prev, n_inc0, n_inc1, n_next, n_p0, n_pn, n_cr, n_cc, n_c0, n_cn, n_m0, n_a0, n_a1,
    ta, tb, tw, isem, osem,
):
    del mis_in
    even = parity() == 0
    cor_e = bulk_e.at[136:160]
    copies = fetch(
        [(inc.at[0], n_inc0), (inc.at[1], n_inc1), (prec.at[0], n_p0), (cr, n_cr), (cc, n_cc)], isem
    )
    own_codes(codes, 0, n_c0, up, dn, 0)
    for j in range(NJ):
        halo(n_inc0, j, blk(up, 0, j), blk(dn, 0, j))
        halo(n_inc1, j, blk(up, 8, j), blk(dn, 8, j))
        halo(n_cr, j, blk(up, 16, j), blk(dn, 16, j))
        halo(n_cc, j, blk(up, 24, j), blk(dn, 24, j))
        halo(n_p0, j, pltpu.roll(blk(up, 16, j), 5, 0), pltpu.roll(blk(dn, 16, j), 3, 0))

    def previous(bulk, cor):
        for j in range(NJ):
            for b in range(8):
                n_prev[j, 8 + 8 * b : 16 + 8 * b] = blk(bulk, 8 * b, j)
            halo(n_prev, j, blk(cor, 0, j), blk(cor, 8, j))

    def following(bulk, cor):
        for j in range(NJ):
            for b in range(8):
                n_next[j, 8 + 8 * b : 16 + 8 * b] = blk(bulk, 8 * b, j)
                n_pn[j, 8 + 8 * b : 16 + 8 * b] = blk(bulk, 64 + 8 * b, j)
                spread(n_cn, j, 8 + 8 * b, bulk[128 + b : 129 + b, j * L : (j + 1) * L])
            halo(n_next, j, blk(cor, 0, j), blk(cor, 8, j))
            spread(n_cn, j, 0, blk(cor, 0, j)[0:1])
            spread(n_cn, j, 72, blk(cor, 8, j)[7:8])
            halo(n_pn, j, pltpu.roll(blk(cor, 16, j), 5, 0), pltpu.roll(blk(cor, 16, j), 3, 0))

    @pl.when(even)
    def _():
        previous(bulk_o, cor_o)
        following(bulk_e, cor_e)

    @pl.when(jnp.logical_not(even))
    def _():
        previous(bulk_e, cor_e)
        following(bulk_o, cor_o)

    for c in copies:
        c.wait()
    wn = (n_cr, n_cc)
    inside = inside_rows()
    misfit_stage(n_prev, n_inc0, n_c0, wn, ta, n_m0)
    outs = emit_out(n_m0, mis.at[0], osem, 0)
    smooth_stages(ta, tb, n_p0, tw, inside)
    for f in range(F):
        for j0 in range(0, NJ, G):
            save(n_a0, f, j0, tw[f, j0 : j0 + G] - image1[f, j0 : j0 + G])
    outs += emit_out(n_a0, adj.at[0], osem, NJ)
    misfit_stage(n_inc1, n_next, n_cn, wn, ta, None)
    smooth_stages(ta, tb, n_pn, tw, inside)
    adjoint_stage(
        tw, n_cn, wn, lambda f, j0, image: save(n_a1, f, j0, w1[f, j0 : j0 + G] - image)
    )
    outs += emit_out(n_a1, adj.at[1], osem, 2 * NJ)
    for c in outs:
        c.wait()


NAT = VMEM((NJ, 80, L), jnp.float32)
TFORM = VMEM((F, NJ, 8, L), jnp.float32)
ON_HBM = pl.BlockSpec(memory_space=pltpu.HBM)
ON_VMEM = pl.BlockSpec(memory_space=VMEM)
OUT = jax.ShapeDtypeStruct((2, 64, 2048), jnp.float32)


def last_step(*args):
    t = jax.ShapeDtypeStruct((F, NJ, 8, L), jnp.float32)
    return pl.pallas_call(
        last_body,
        in_specs=[ON_HBM] * 4 + [ON_VMEM] * 3,
        out_specs=[ON_HBM] + [ON_VMEM] * 2,
        out_shape=[OUT, t, t],
        scratch_shapes=[NAT] * 7
        + [TFORM] * 3
        + [pltpu.SemaphoreType.DMA((5 * NJ,)), pltpu.SemaphoreType.DMA((NJ,))],
        compiler_params=pltpu.CompilerParams(vmem_limit_bytes=24 << 20),
        name="last",
    )(*args)


def first_steps(*args):
    return pl.pallas_call(
        first_body,
        in_specs=[ON_HBM] * 4 + [ON_VMEM] * 8 + [ON_HBM],
        out_specs=[ON_HBM] * 2,
        out_shape=[OUT, OUT],
        scratch_shapes=[NAT] * 13
        + [TFORM] * 3
        + [pltpu.SemaphoreType.DMA((5 * NJ,)), pltpu.SemaphoreType.DMA((3 * NJ,))],
        input_output_aliases={12: 0},
        compiler_params=pltpu.CompilerParams(vmem_limit_bytes=24 << 20),
        name="first",
    )(*args)


def permute(x, rule):
    axes = ("tm", "space")
    nt, ns = lax.axis_size("tm"), lax.axis_size("space")
    pairs = []
    for t in range(nt):
        for s in range(ns):
            a, b = rule(t, s)
            if 0 <= a < nt and 0 <= b < ns:
                pairs.append((t * ns + s, a * ns + b))
    return lax.ppermute(x, axes, pairs)


def off_chip(t, s):
    return (t - 1 if t % 2 == 0 else t + 1), s


def on_chip(t, s):
    return (t + 1 if t % 2 == 0 else t - 1), s


def on_device(inc, prec, cr, cc, codes):
    bulk_o, bulk_e, up, dn = pack(inc, prec, cr, cc, codes)
    up = permute(up, lambda t, s: (t, s + 1))
    bulk_o = permute(bulk_o, off_chip)
    dn = permute(dn, lambda t, s: (t, s - 1))
    cor_o, bulk_e = corner(up, dn, bulk_e)
    cor_o = permute(cor_o, off_chip)
    bulk_e = permute(bulk_e, on_chip)
    mis, w1, image1 = last_step(inc, prec, cr, cc, codes, up, dn)
    return tuple(
        first_steps(
            inc, prec, cr, cc, codes, up, dn, bulk_o, bulk_e, cor_o, w1, image1, mis
        )
    )


def solution(mesh):
    in_specs = (
        P("tm", "space", None),
        P("tm", "space", None),
        P("space", None),
        P("space", None),
        P("tm", "space", None),
    )
    out_specs = (P("tm", "space", None), P("tm", "space", None))
    return jax.shard_map(
        on_device, mesh=mesh, in_specs=in_specs, out_specs=out_specs, check_vma=False
    )
```

```python
import jax
import jax.numpy as jnp
from jax import lax
from jax.experimental import pallas as pl
from jax.experimental.pallas import tpu as pltpu
from jax.sharding import PartitionSpec as P


F = 10
NJ = 16
G = 4
L = 128
C4 = 0.04 * 0.04
VMEM = pltpu.VMEM


def lanes():
    return lax.broadcasted_iota(jnp.int32, (1, 8, L), 2)


def sublanes(shape):
    return lax.broadcasted_iota(jnp.int32, shape, len(shape) - 2)


def load(nat, f, j0, n):
    return jnp.stack([nat[(j0 + g) % NJ, pl.ds(f, 8, stride=F), :] for g in range(n)])


def save(nat, f, j0, x):
    for g in range(G):
        nat[j0 + g, pl.ds(f, 8, stride=F), :] = x[g]


def load_t(t, f, j0, n):
    parts = []
    if j0 < 0:
        parts.append(t[f, NJ - 1 : NJ])
    parts.append(t[f, max(j0, 0) : min(j0 + n, NJ)])
    if j0 + n > NJ:
        parts.append(t[f, 0:1])
    return parts[0] if len(parts) == 1 else jnp.concatenate(parts, axis=0)


def beside(u):
    first = lanes() == 0
    last = lanes() == L - 1
    right_of = pltpu.roll(u[: G + 1], 1, 2)
    left_of = pltpu.roll(u[1:], L - 1, 2)
    left = jnp.where(first, right_of[:G], right_of[1:])
    right = jnp.where(last, left_of[1:], left_of[:G])
    return left, right


def masks(code):
    mc = code < 1.5
    mr = jnp.where(mc, code, code - 2.0) < 0.5
    return mr, mc


def stencil(get, visit):
    for j0 in range(0, NJ, G):
        above = pltpu.roll(get(F - 1, j0, G), 1, 1)
        wide = get(0, j0 - 1, G + 2)
        for f in range(F):
            if f < F - 1:
                after = get(f + 1, j0 - 1, G + 2)
                below = after[1 : G + 1]
            else:
                after = None
                below = pltpu.roll(get(0, j0, G), 7, 1)
            visit(f, j0, wide, above, below)
            above = wide[1 : G + 1]
            wide = after


def misfit_stage(un, vn, code, wn, tout, out):
    def visit(f, j0, u, up, down):
        left, right = beside(u)
        mr, mc = masks(load(code, f, j0, G))
        cr, cc = load(wn[0], f, j0, G), load(wn[1], f, j0, G)
        moved = (
            (1.0 - cr - cc) * u[1 : G + 1]
            + cr * jnp.where(mr, up, down)
            + cc * jnp.where(mc, left, right)
        )
        mis = load(vn, f, j0, G) - moved
        tout[f, j0 : j0 + G] = mis
        if out is not None:
            save(out, f, j0, mis)

    stencil(lambda f, j0, n: load(un, f, j0, n), visit)


def sweep_stage(tin, tout, after):
    def visit(f, j0, u, up, down):
        left, right = beside(u)
        x = ((up + down) + (left + right)) + u[1 : G + 1]
        tout[f, j0 : j0 + G] = after(x, f, j0)

    stencil(lambda f, j0, n: load_t(tin, f, j0, n), visit)


def smooth_stages(tin, tmp, pn, tout, inside):
    def mask(x, f, j0):
        return jnp.where(inside(f), x, 0.0)

    def scale(x, f, j0):
        return (load(pn, f, j0, G) * C4) * x

    sweep_stage(tin, tmp, mask)
    sweep_stage(tmp, tin, scale)
    sweep_stage(tin, tmp, mask)
    sweep_stage(tmp, tout, lambda x, f, j0: x)


def adjoint_stage(tw, code, wn, emit):
    first = lanes() == 0
    last = lanes() == L - 1

    def pieces(f, j0):
        w = load_t(tw, f, j0 - 1, G + 2)
        mr, mc = masks(load(code, f, j0 - 1, G + 2))
        mr = mr[1 : G + 1]
        cr = load(wn[0], f, j0, G)
        cc = load(wn[1], f, j0 - 1, G + 2)
        mid = w[1 : G + 1]
        rows = cr * mid
        lower = jnp.where(mr, rows, 0.0)
        cols = cc * w
        plus = pltpu.roll(jnp.where(mc, cols, 0.0)[1:], L - 1, 2)
        minus = pltpu.roll(jnp.where(mc, 0.0, cols)[: G + 1], 1, 2)
        image = (
            (1.0 - cr - cc[1 : G + 1]) * mid
            + jnp.where(last, plus[1:], plus[:G])
            + jnp.where(first, minus[:G], minus[1:])
        )
        return image, lower, rows - lower

    def upper_only(f, j0):
        mr, _ = masks(load(code, f, j0, G))
        return jnp.where(mr, 0.0, load(wn[0], f, j0, G) * load_t(tw, f, j0, G))

    for j0 in range(0, NJ, G):
        above = pltpu.roll(upper_only(F - 1, j0), 1, 1)
        image, lower, upper = pieces(0, j0)
        lower0 = pltpu.roll(lower, 7, 1)
        for f in range(F):
            if f < F - 1:
                after = pieces(f + 1, j0)
                below = after[1]
            else:
                after = None
                below = lower0
            emit(f, j0, image + (above + below))
            above = upper
            if after is not None:
                image, lower, upper = after


def parity():
    return lax.axis_index("tm") % 2


def code_rows(codes, step):
    c = codes[step].astype(jnp.float32)
    return [jnp.broadcast_to(c[:, j : j + 1], (8, L)) for j in range(NJ)]


def pack_kernel(copies, inc, prec, edge, codes, bulk_o, bulk_e, pass_1, pass_2, sems):
    even = parity() == 0

    def forward(dst):
        return [pltpu.make_async_copy(inc.at[1], dst.at[pl.ds(0, 64)], sems.at[0])]

    def backward(dst):
        return [
            pltpu.make_async_copy(inc.at[0], dst.at[pl.ds(0, 64)], sems.at[1]),
            pltpu.make_async_copy(prec.at[0], dst.at[pl.ds(64, 64)], sems.at[2]),
        ]

    def start(fwd, bwd):
        for c in forward(fwd) + backward(bwd):
            c.start()

    @pl.when(even)
    def _():
        start(bulk_e, bulk_o)

    @pl.when(jnp.logical_not(even))
    def _():
        start(bulk_o, bulk_e)

    for c in copies:
        c.wait()
    row = sublanes((8, L))
    rows0 = code_rows(codes, 0)
    rows1 = code_rows(codes, 1)
    for j in range(NJ):
        cols = pl.ds(j * L, L)
        bulk_o[128:136, cols] = rows0[j]
        bulk_e[128:136, cols] = rows0[j]

    def edges(up, dn):
        for j in range(NJ):
            cols = pl.ds(j * L, L)
            inc0t, inc0b, inc1t, inc1b, p0t, p0b, p1t, p1b, crt, crb, cct, ccb = [
                edge[k, :, cols] for k in range(12)
            ]
            c0t = jnp.broadcast_to(rows0[j][0:1], (8, L))
            c0b = jnp.broadcast_to(rows0[j][7:8], (8, L))
            c1t = jnp.broadcast_to(rows1[j][0:1], (8, L))
            c1b = jnp.broadcast_to(rows1[j][7:8], (8, L))
            up[0:8, cols] = jnp.where(row < 2, c0b, inc0b)
            up[8:16, cols] = jnp.where(row < 2, c1b, inc1b)
            up[16:24, cols] = jnp.where(row < 3, pltpu.roll(p0b, 3, 0), crb)
            up[24:32, cols] = jnp.where(row < 3, pltpu.roll(p1b, 3, 0), ccb)
            dn[0:8, cols] = jnp.where(row > 5, c0t, inc0t)
            dn[8:16, cols] = jnp.where(row > 5, c1t, inc1t)
            dn[16:24, cols] = jnp.where(row > 4, pltpu.roll(p0t, 5, 0), crt)
            dn[24:32, cols] = jnp.where(row > 4, pltpu.roll(p1t, 5, 0), cct)

    @pl.when(even)
    def _():
        edges(pass_1, pass_2)

    @pl.when(jnp.logical_not(even))
    def _():
        edges(pass_2, pass_1)

    @pl.when(even)
    def _():
        for c in forward(bulk_e) + backward(bulk_o):
            c.wait()

    @pl.when(jnp.logical_not(even))
    def _():
        for c in forward(bulk_o) + backward(bulk_e):
            c.wait()


def pack_body(inc, prec, cr, cc, codes_hbm, bulk_o, bulk_e, pass_1, pass_2, codes, edge, sems, esems):
    top, bottom = pl.ds(0, 8), pl.ds(56, 8)
    srcs = []
    for a in (inc.at[0], inc.at[1], prec.at[0], prec.at[1], cr, cc):
        srcs += [a.at[top], a.at[bottom]]
    copies = [pltpu.make_async_copy(codes_hbm, codes, esems.at[12])]
    copies += [pltpu.make_async_copy(s, edge.at[k], esems.at[k]) for k, s in enumerate(srcs)]
    for c in copies:
        c.start()
    pack_kernel(copies, inc, prec, edge, codes, bulk_o, bulk_e, pass_1, pass_2, sems)


def pack(inc, prec, cr, cc, codes):
    any_spec = pl.BlockSpec(memory_space=pltpu.HBM)
    vmem = pl.BlockSpec(memory_space=VMEM)
    f32 = lambda *s: jax.ShapeDtypeStruct(s, jnp.float32)
    return pl.pallas_call(
        pack_body,
        in_specs=[any_spec] * 5,
        out_specs=[vmem] * 4,
        out_shape=[f32(136, 2048), f32(160, 2048), f32(32, 2048), f32(32, 2048)],
        scratch_shapes=[
            VMEM((2, 8, 16), jnp.int32),
            VMEM((12, 8, 2048), jnp.float32),
            pltpu.SemaphoreType.DMA((3,)),
            pltpu.SemaphoreType.DMA((13,)),
        ],
        compiler_params=pltpu.CompilerParams(vmem_limit_bytes=12 << 20),
        name="pack",
    )(*(pltpu.with_memory_space_constraint(a, pltpu.HBM) for a in (inc, prec, cr, cc, codes)))


def corner_body(pass_1, pass_2, bulk_in, up, dn, cor_o, bulk_e):
    del bulk_in
    cor_e = bulk_e.at[136:160]
    even = parity() == 0
    row = sublanes((8, 2048))

    def forward(up, dn, dst):
        dst[0:8, :] = up[8:16, :]
        dst[8:16, :] = dn[8:16, :]
        dst[16:24, :] = up[8:16, :]

    def backward(up, dn, dst):
        dst[0:8, :] = up[0:8, :]
        dst[8:16, :] = dn[0:8, :]
        dst[16:24, :] = jnp.where(row < 4, up[16:24, :], dn[16:24, :])

    def both(from_up, from_dn, fwd, bwd):
        up[...] = from_up[...]
        dn[...] = from_dn[...]
        forward(from_up, from_dn, fwd)
        backward(from_up, from_dn, bwd)

    @pl.when(even)
    def _():
        both(pass_1, pass_2, cor_e, cor_o)

    @pl.when(jnp.logical_not(even))
    def _():
        both(pass_2, pass_1, cor_o, cor_e)


def corner(pass_1, pass_2, bulk_e):
    vmem = pl.BlockSpec(memory_space=VMEM)
    f32 = lambda *s: jax.ShapeDtypeStruct(s, jnp.float32)
    return pl.pallas_call(
        corner_body,
        in_specs=[vmem] * 2 + [pl.BlockSpec(memory_space=pl.ANY)],
        out_specs=[vmem] * 4,
        out_shape=[f32(32, 2048), f32(32, 2048), f32(24, 2048), f32(160, 2048)],
        input_output_aliases={2: 3},
        compiler_params=pltpu.CompilerParams(vmem_limit_bytes=8 << 20),
        name="corner",
    )(pass_1, pass_2, bulk_e)


def blk(ref, r, j):
    return ref[r : r + 8, j * L : (j + 1) * L]


def spread(dst, j, at, x):
    dst[j, at : at + 8] = jnp.broadcast_to(x, (8, L))


def halo(dst, j, top, bottom):
    dst[j, 0:8] = top
    dst[j, 72:80] = bottom


def fill(src, dst):
    for j in range(NJ):
        for b in range(8):
            dst[j, 8 + 8 * b : 16 + 8 * b] = src[8 * b : 8 * b + 8, j * L : (j + 1) * L]


def emit_out(nat, dst, sem, base):
    copies = [
        pltpu.make_async_copy(
            nat.at[j, pl.ds(8, 64)], dst.at[:, pl.ds(j * L, L)], sem.at[base + j]
        )
        for j in range(NJ)
    ]
    for c in copies:
        c.start()
    return copies


def inside_rows():
    slab = lax.axis_index("space")
    sub = sublanes((1, 8, L))
    top_out = (sub == 0) & (slab == 0)
    bottom_out = (sub == 7) & (slab == lax.axis_size("space") - 1)

    def inside(f):
        bad = None
        if f < 8:
            bad = top_out
        if f >= 2:
            bad = bottom_out if bad is None else bad | bottom_out
        return jnp.logical_not(bad)

    return inside


def own_codes(codes, step, n_c, up, dn, r):
    rows = code_rows(codes, step)
    for j in range(NJ):
        for b in range(8):
            spread(n_c, j, 8 + 8 * b, rows[j][b : b + 1])
        spread(n_c, j, 0, blk(up, r, j)[0:1])
        spread(n_c, j, 72, blk(dn, r, j)[7:8])


def last_body(
    inc, prec, cr, cc, codes, up, dn, mis, w_out, image_out, n_inc0, n_inc1, n_cr, n_cc,
    n_p1, n_c1, n_m1, ta, tb, tw, osem,
):
    for src, dst in (
        (inc.at[0], n_inc0), (inc.at[1], n_inc1), (prec.at[1], n_p1), (cr, n_cr), (cc, n_cc)
    ):
        fill(src, dst)
    own_codes(codes, 1, n_c1, up, dn, 8)
    for j in range(NJ):
        halo(n_inc0, j, blk(up, 0, j), blk(dn, 0, j))
        halo(n_inc1, j, blk(up, 8, j), blk(dn, 8, j))
        halo(n_cr, j, blk(up, 16, j), blk(dn, 16, j))
        halo(n_cc, j, blk(up, 24, j), blk(dn, 24, j))
        halo(n_p1, j, pltpu.roll(blk(up, 24, j), 5, 0), pltpu.roll(blk(dn, 24, j), 3, 0))
    wn = (n_cr, n_cc)
    inside = inside_rows()
    misfit_stage(n_inc0, n_inc1, n_c1, wn, ta, n_m1)
    outs = emit_out(n_m1, mis.at[1], osem, 0)
    smooth_stages(ta, tb, n_p1, tw, inside)

    def emit(f, j0, image):
        image_out[f, j0 : j0 + G] = image
        w_out[f, j0 : j0 + G] = tw[f, j0 : j0 + G]

    adjoint_stage(tw, n_c1, wn, emit)
    for c in outs:
        c.wait()


def first_body(
    prec, codes, up, dn, bulk_o, bulk_e, cor_o, w1, image1, n_inc0, n_inc1, n_cr, n_cc, mis_in,
    mis, adj,
    n_prev, n_next, n_p0, n_pn, n_c0, n_cn, n_m0, n_a0, n_a1, ta, tb, tw, osem,
):
    del mis_in
    even = parity() == 0
    cor_e = bulk_e.at[136:160]
    fill(prec.at[0], n_p0)
    own_codes(codes, 0, n_c0, up, dn, 0)
    for j in range(NJ):
        halo(n_p0, j, pltpu.roll(blk(up, 16, j), 5, 0), pltpu.roll(blk(dn, 16, j), 3, 0))

    def previous(bulk, cor):
        for j in range(NJ):
            for b in range(8):
                n_prev[j, 8 + 8 * b : 16 + 8 * b] = blk(bulk, 8 * b, j)
            halo(n_prev, j, blk(cor, 0, j), blk(cor, 8, j))

    def following(bulk, cor):
        for j in range(NJ):
            for b in range(8):
                n_next[j, 8 + 8 * b : 16 + 8 * b] = blk(bulk, 8 * b, j)
                n_pn[j, 8 + 8 * b : 16 + 8 * b] = blk(bulk, 64 + 8 * b, j)
                spread(n_cn, j, 8 + 8 * b, bulk[128 + b : 129 + b, j * L : (j + 1) * L])
            halo(n_next, j, blk(cor, 0, j), blk(cor, 8, j))
            spread(n_cn, j, 0, blk(cor, 0, j)[0:1])
            spread(n_cn, j, 72, blk(cor, 8, j)[7:8])
            halo(n_pn, j, pltpu.roll(blk(cor, 16, j), 5, 0), pltpu.roll(blk(cor, 16, j), 3, 0))

    @pl.when(even)
    def _():
        previous(bulk_o, cor_o)
        following(bulk_e, cor_e)

    @pl.when(jnp.logical_not(even))
    def _():
        previous(bulk_e, cor_e)
        following(bulk_o, cor_o)

    wn = (n_cr, n_cc)
    inside = inside_rows()
    misfit_stage(n_prev, n_inc0, n_c0, wn, ta, n_m0)
    outs = emit_out(n_m0, mis.at[0], osem, 0)
    smooth_stages(ta, tb, n_p0, tw, inside)
    for f in range(F):
        for j0 in range(0, NJ, G):
            save(n_a0, f, j0, tw[f, j0 : j0 + G] - image1[f, j0 : j0 + G])
    outs += emit_out(n_a0, adj.at[0], osem, NJ)
    misfit_stage(n_inc1, n_next, n_cn, wn, ta, None)
    smooth_stages(ta, tb, n_pn, tw, inside)
    adjoint_stage(
        tw, n_cn, wn, lambda f, j0, image: save(n_a1, f, j0, w1[f, j0 : j0 + G] - image)
    )
    outs += emit_out(n_a1, adj.at[1], osem, 2 * NJ)
    for c in outs:
        c.wait()


NAT = VMEM((NJ, 80, L), jnp.float32)
TFORM = VMEM((F, NJ, 8, L), jnp.float32)
ON_HBM = pl.BlockSpec(memory_space=pltpu.HBM)
ON_VMEM = pl.BlockSpec(memory_space=VMEM)
OUT = jax.ShapeDtypeStruct((2, 64, 2048), jnp.float32)


def last_step(*args):
    t = jax.ShapeDtypeStruct((F, NJ, 8, L), jnp.float32)
    n = jax.ShapeDtypeStruct((NJ, 80, L), jnp.float32)
    return pl.pallas_call(
        last_body,
        in_specs=[ON_VMEM] * 7,
        out_specs=[ON_HBM] + [ON_VMEM] * 6,
        out_shape=[OUT, t, t, n, n, n, n],
        scratch_shapes=[NAT] * 3 + [TFORM] * 3 + [pltpu.SemaphoreType.DMA((NJ,))],
        compiler_params=pltpu.CompilerParams(vmem_limit_bytes=24 << 20),
        name="last",
    )(*args)


def first_steps(*args):
    return pl.pallas_call(
        first_body,
        in_specs=[ON_VMEM] * 13 + [ON_HBM],
        out_specs=[ON_HBM] * 2,
        out_shape=[OUT, OUT],
        scratch_shapes=[NAT] * 9 + [TFORM] * 3 + [pltpu.SemaphoreType.DMA((3 * NJ,))],
        input_output_aliases={13: 0},
        compiler_params=pltpu.CompilerParams(vmem_limit_bytes=24 << 20),
        name="first",
    )(*args)


def permute(x, rule):
    axes = ("tm", "space")
    nt, ns = lax.axis_size("tm"), lax.axis_size("space")
    pairs = []
    for t in range(nt):
        for s in range(ns):
            a, b = rule(t, s)
            if 0 <= a < nt and 0 <= b < ns:
                pairs.append((t * ns + s, a * ns + b))
    return lax.ppermute(x, axes, pairs)


def off_chip(t, s):
    return (t - 1 if t % 2 == 0 else t + 1), s


def on_chip(t, s):
    return (t + 1 if t % 2 == 0 else t - 1), s


def up_on_even(t, s):
    return t, (s + 1 if t % 2 == 0 else s - 1)


def down_on_even(t, s):
    return t, (s - 1 if t % 2 == 0 else s + 1)


def on_device(inc, prec, cr, cc, codes):
    bulk_o, bulk_e, pass_1, pass_2 = pack(inc, prec, cr, cc, codes)
    bulk_o = permute(bulk_o, off_chip)
    pass_1 = permute(pass_1, up_on_even)
    pass_2 = permute(pass_2, down_on_even)
    up, dn, cor_o, bulk_e = corner(pass_1, pass_2, bulk_e)
    cor_o = permute(cor_o, off_chip)
    bulk_e = permute(bulk_e, on_chip)
    mis, *kept = last_step(inc, prec, cr, cc, codes, up, dn)
    return tuple(first_steps(prec, codes, up, dn, bulk_o, bulk_e, cor_o, *kept, mis))


def solution(mesh):
    in_specs = (
        P("tm", "space", None),
        P("tm", "space", None),
        P("space", None),
        P("space", None),
        P("tm", "space", None),
    )
    out_specs = (P("tm", "space", None), P("tm", "space", None))
    return jax.shard_map(
        on_device, mesh=mesh, in_specs=in_specs, out_specs=out_specs, check_vma=False
    )
```

```python
import jax
import jax.numpy as jnp
from jax import lax
from jax.experimental import pallas as pl
from jax.experimental.pallas import tpu as pltpu
from jax.sharding import PartitionSpec as P


F = 10
NJ = 16
G = 4
L = 128
C4 = 0.04 * 0.04
VMEM = pltpu.VMEM


def lanes():
    return lax.broadcasted_iota(jnp.int32, (1, 8, L), 2)


def sublanes(shape):
    return lax.broadcasted_iota(jnp.int32, shape, len(shape) - 2)


def load(nat, f, j0, n):
    return jnp.stack([nat[(j0 + g) % NJ, pl.ds(f, 8, stride=F), :] for g in range(n)])


def save(nat, f, j0, x):
    for g in range(G):
        nat[j0 + g, pl.ds(f, 8, stride=F), :] = x[g]


def load_t(t, f, j0, n):
    parts = []
    if j0 < 0:
        parts.append(t[f, NJ - 1 : NJ])
    parts.append(t[f, max(j0, 0) : min(j0 + n, NJ)])
    if j0 + n > NJ:
        parts.append(t[f, 0:1])
    return parts[0] if len(parts) == 1 else jnp.concatenate(parts, axis=0)


def masks(code):
    mc = code < 1.5
    mr = jnp.where(mc, code, code - 2.0) < 0.5
    return mr, mc


def stencil(get, visit):
    first = lanes() == 0
    last = lanes() == L - 1
    for f in range(F):
        before = pltpu.roll(get(f, NJ - 1, 1), 1, 2)
        here = get(f, 0, G)
        back = pltpu.roll(here, L - 1, 2)
        start = back[:1]
        for j0 in range(0, NJ, G):
            if j0 + G < NJ:
                there = get(f, j0 + G, G)
                back_there = pltpu.roll(there, L - 1, 2)
                edge = back_there[:1]
            else:
                there = back_there = None
                edge = start
            fore = pltpu.roll(here, 1, 2)
            left = jnp.where(first, jnp.concatenate([before, fore[: G - 1]], axis=0), fore)
            right = jnp.where(last, jnp.concatenate([back[1:], edge], axis=0), back)
            above = get(f - 1, j0, G) if f > 0 else pltpu.roll(get(F - 1, j0, G), 1, 1)
            below = get(f + 1, j0, G) if f < F - 1 else pltpu.roll(get(0, j0, G), 7, 1)
            visit(f, j0, here, left, right, above, below)
            before = fore[G - 1 :]
            here, back = there, back_there


def misfit_stage(un, vn, code, wn, tout, out):
    def visit(f, j0, u, left, right, up, down):
        mr, mc = masks(load(code, f, j0, G))
        cr, cc = load(wn[0], f, j0, G), load(wn[1], f, j0, G)
        moved = (
            (1.0 - cr - cc) * u
            + cr * jnp.where(mr, up, down)
            + cc * jnp.where(mc, left, right)
        )
        mis = load(vn, f, j0, G) - moved
        tout[f, j0 : j0 + G] = mis
        if out is not None:
            save(out, f, j0, mis)

    stencil(lambda f, j0, n: load(un, f, j0, n), visit)


def sweep_stage(tin, tout, after):
    def visit(f, j0, u, left, right, up, down):
        x = ((up + down) + (left + right)) + u
        tout[f, j0 : j0 + G] = after(x, f, j0)

    stencil(lambda f, j0, n: load_t(tin, f, j0, n), visit)


def smooth_stages(tin, tmp, pn, tout, inside):
    def mask(x, f, j0):
        return jnp.where(inside(f), x, 0.0)

    def scale(x, f, j0):
        return (load(pn, f, j0, G) * C4) * x

    sweep_stage(tin, tmp, mask)
    sweep_stage(tmp, tin, scale)
    sweep_stage(tin, tmp, mask)
    sweep_stage(tmp, tout, lambda x, f, j0: x)


def adjoint_stage(tw, code, wn, emit):
    first = lanes() == 0
    last = lanes() == L - 1

    def pieces(f, j0):
        w = load_t(tw, f, j0 - 1, G + 2)
        mr, mc = masks(load(code, f, j0 - 1, G + 2))
        mr = mr[1 : G + 1]
        cr = load(wn[0], f, j0, G)
        cc = load(wn[1], f, j0 - 1, G + 2)
        mid = w[1 : G + 1]
        rows = cr * mid
        lower = jnp.where(mr, rows, 0.0)
        cols = cc * w
        plus = pltpu.roll(jnp.where(mc, cols, 0.0)[1:], L - 1, 2)
        minus = pltpu.roll(jnp.where(mc, 0.0, cols)[: G + 1], 1, 2)
        image = (
            (1.0 - cr - cc[1 : G + 1]) * mid
            + jnp.where(last, plus[1:], plus[:G])
            + jnp.where(first, minus[:G], minus[1:])
        )
        return image, lower, rows - lower

    def upper_only(f, j0):
        mr, _ = masks(load(code, f, j0, G))
        return jnp.where(mr, 0.0, load(wn[0], f, j0, G) * load_t(tw, f, j0, G))

    for j0 in range(0, NJ, G):
        above = pltpu.roll(upper_only(F - 1, j0), 1, 1)
        image, lower, upper = pieces(0, j0)
        lower0 = pltpu.roll(lower, 7, 1)
        for f in range(F):
            if f < F - 1:
                after = pieces(f + 1, j0)
                below = after[1]
            else:
                after = None
                below = lower0
            emit(f, j0, image + (above + below))
            above = upper
            if after is not None:
                image, lower, upper = after


def parity():
    return lax.axis_index("tm") % 2


def code_rows(codes, step):
    c = codes[step].astype(jnp.float32)
    return [jnp.broadcast_to(c[:, j : j + 1], (8, L)) for j in range(NJ)]


def pack_kernel(copies, inc, prec, edge, codes, bulk_o, bulk_e, pass_1, pass_2, sems):
    even = parity() == 0

    def forward(dst):
        return [pltpu.make_async_copy(inc.at[1], dst.at[pl.ds(0, 64)], sems.at[0])]

    def backward(dst):
        return [
            pltpu.make_async_copy(inc.at[0], dst.at[pl.ds(0, 64)], sems.at[1]),
            pltpu.make_async_copy(prec.at[0], dst.at[pl.ds(64, 64)], sems.at[2]),
        ]

    def start(fwd, bwd):
        for c in forward(fwd) + backward(bwd):
            c.start()

    @pl.when(even)
    def _():
        start(bulk_e, bulk_o)

    @pl.when(jnp.logical_not(even))
    def _():
        start(bulk_o, bulk_e)

    for c in copies:
        c.wait()
    row = sublanes((8, L))
    rows0 = code_rows(codes, 0)
    rows1 = code_rows(codes, 1)
    for j in range(NJ):
        cols = pl.ds(j * L, L)
        bulk_o[128:136, cols] = rows0[j]
        bulk_e[128:136, cols] = rows0[j]

    def edges(up, dn):
        for j in range(NJ):
            cols = pl.ds(j * L, L)
            inc0t, inc0b, inc1t, inc1b, p0t, p0b, p1t, p1b, crt, crb, cct, ccb = [
                edge[k, :, cols] for k in range(12)
            ]
            c0t = jnp.broadcast_to(rows0[j][0:1], (8, L))
            c0b = jnp.broadcast_to(rows0[j][7:8], (8, L))
            c1t = jnp.broadcast_to(rows1[j][0:1], (8, L))
            c1b = jnp.broadcast_to(rows1[j][7:8], (8, L))
            up[0:8, cols] = jnp.where(row < 2, c0b, inc0b)
            up[8:16, cols] = jnp.where(row < 2, c1b, inc1b)
            up[16:24, cols] = jnp.where(row < 3, pltpu.roll(p0b, 3, 0), crb)
            up[24:32, cols] = jnp.where(row < 3, pltpu.roll(p1b, 3, 0), ccb)
            dn[0:8, cols] = jnp.where(row > 5, c0t, inc0t)
            dn[8:16, cols] = jnp.where(row > 5, c1t, inc1t)
            dn[16:24, cols] = jnp.where(row > 4, pltpu.roll(p0t, 5, 0), crt)
            dn[24:32, cols] = jnp.where(row > 4, pltpu.roll(p1t, 5, 0), cct)

    edges(pass_1, pass_2)

    @pl.when(even)
    def _():
        for c in forward(bulk_e) + backward(bulk_o):
            c.wait()

    @pl.when(jnp.logical_not(even))
    def _():
        for c in forward(bulk_o) + backward(bulk_e):
            c.wait()


def pack_body(inc, prec, cr, cc, codes_hbm, bulk_o, bulk_e, pass_1, pass_2, codes, edge, sems, esems):
    top, bottom = pl.ds(0, 8), pl.ds(56, 8)
    srcs = []
    for a in (inc.at[0], inc.at[1], prec.at[0], prec.at[1], cr, cc):
        srcs += [a.at[top], a.at[bottom]]
    copies = [pltpu.make_async_copy(codes_hbm, codes, esems.at[12])]
    copies += [pltpu.make_async_copy(s, edge.at[k], esems.at[k]) for k, s in enumerate(srcs)]
    for c in copies:
        c.start()
    pack_kernel(copies, inc, prec, edge, codes, bulk_o, bulk_e, pass_1, pass_2, sems)


def pack(inc, prec, cr, cc, codes):
    any_spec = pl.BlockSpec(memory_space=pltpu.HBM)
    vmem = pl.BlockSpec(memory_space=VMEM)
    f32 = lambda *s: jax.ShapeDtypeStruct(s, jnp.float32)
    return pl.pallas_call(
        pack_body,
        in_specs=[any_spec] * 5,
        out_specs=[vmem] * 4,
        out_shape=[f32(136, 2048), f32(160, 2048), f32(32, 2048), f32(32, 2048)],
        scratch_shapes=[
            VMEM((2, 8, 16), jnp.int32),
            VMEM((12, 8, 2048), jnp.float32),
            pltpu.SemaphoreType.DMA((3,)),
            pltpu.SemaphoreType.DMA((13,)),
        ],
        compiler_params=pltpu.CompilerParams(vmem_limit_bytes=12 << 20),
        name="pack",
    )(*(pltpu.with_memory_space_constraint(a, pltpu.HBM) for a in (inc, prec, cr, cc, codes)))


def corner_body(pass_1, pass_2, bulk_in, up, dn, cor_o, bulk_e):
    del bulk_in
    cor_e = bulk_e.at[136:160]
    even = parity() == 0
    row = sublanes((8, 2048))

    def forward(up, dn, dst):
        dst[0:8, :] = up[8:16, :]
        dst[8:16, :] = dn[8:16, :]
        dst[16:24, :] = up[8:16, :]

    def backward(up, dn, dst):
        dst[0:8, :] = up[0:8, :]
        dst[8:16, :] = dn[0:8, :]
        dst[16:24, :] = jnp.where(row < 4, up[16:24, :], dn[16:24, :])

    def both(from_up, from_dn, fwd, bwd):
        up[...] = from_up[...]
        dn[...] = from_dn[...]
        forward(from_up, from_dn, fwd)
        backward(from_up, from_dn, bwd)

    @pl.when(even)
    def _():
        both(pass_1, pass_2, cor_e, cor_o)

    @pl.when(jnp.logical_not(even))
    def _():
        both(pass_1, pass_2, cor_o, cor_e)


def corner(pass_1, pass_2, bulk_e):
    vmem = pl.BlockSpec(memory_space=VMEM)
    f32 = lambda *s: jax.ShapeDtypeStruct(s, jnp.float32)
    return pl.pallas_call(
        corner_body,
        in_specs=[vmem] * 2 + [pl.BlockSpec(memory_space=pl.ANY)],
        out_specs=[vmem] * 4,
        out_shape=[f32(32, 2048), f32(32, 2048), f32(24, 2048), f32(160, 2048)],
        input_output_aliases={2: 3},
        compiler_params=pltpu.CompilerParams(vmem_limit_bytes=8 << 20),
        name="corner",
    )(pass_1, pass_2, bulk_e)


def blk(ref, r, j):
    return ref[r : r + 8, j * L : (j + 1) * L]


def spread(dst, j, at, x):
    dst[j, at : at + 8] = jnp.broadcast_to(x, (8, L))


def halo(dst, j, top, bottom):
    dst[j, 0:8] = top
    dst[j, 72:80] = bottom


def fill(src, dst):
    for j in range(NJ):
        for b in range(8):
            dst[j, 8 + 8 * b : 16 + 8 * b] = src[8 * b : 8 * b + 8, j * L : (j + 1) * L]


def emit_out(nat, dst, sem, base):
    copies = [
        pltpu.make_async_copy(
            nat.at[j, pl.ds(8, 64)], dst.at[:, pl.ds(j * L, L)], sem.at[base + j]
        )
        for j in range(NJ)
    ]
    for c in copies:
        c.start()
    return copies


def inside_rows():
    slab = lax.axis_index("space")
    sub = sublanes((1, 8, L))
    top_out = (sub == 0) & (slab == 0)
    bottom_out = (sub == 7) & (slab == lax.axis_size("space") - 1)

    def inside(f):
        bad = None
        if f < 8:
            bad = top_out
        if f >= 2:
            bad = bottom_out if bad is None else bad | bottom_out
        return jnp.logical_not(bad)

    return inside


def own_codes(codes, step, n_c, up, dn, r):
    rows = code_rows(codes, step)
    for j in range(NJ):
        for b in range(8):
            spread(n_c, j, 8 + 8 * b, rows[j][b : b + 1])
        spread(n_c, j, 0, blk(up, r, j)[0:1])
        spread(n_c, j, 72, blk(dn, r, j)[7:8])


def last_body(
    inc, prec, cr, cc, codes, up, dn, mis, w_out, image_out, n_inc0, n_inc1, n_cr, n_cc,
    n_p1, n_c1, n_m1, ta, tb, tw, osem,
):
    for src, dst in (
        (inc.at[0], n_inc0), (inc.at[1], n_inc1), (prec.at[1], n_p1), (cr, n_cr), (cc, n_cc)
    ):
        fill(src, dst)
    own_codes(codes, 1, n_c1, up, dn, 8)
    for j in range(NJ):
        halo(n_inc0, j, blk(up, 0, j), blk(dn, 0, j))
        halo(n_inc1, j, blk(up, 8, j), blk(dn, 8, j))
        halo(n_cr, j, blk(up, 16, j), blk(dn, 16, j))
        halo(n_cc, j, blk(up, 24, j), blk(dn, 24, j))
        halo(n_p1, j, pltpu.roll(blk(up, 24, j), 5, 0), pltpu.roll(blk(dn, 24, j), 3, 0))
    wn = (n_cr, n_cc)
    inside = inside_rows()
    misfit_stage(n_inc0, n_inc1, n_c1, wn, ta, n_m1)
    outs = emit_out(n_m1, mis.at[1], osem, 0)
    smooth_stages(ta, tb, n_p1, tw, inside)

    def emit(f, j0, image):
        image_out[f, j0 : j0 + G] = image
        w_out[f, j0 : j0 + G] = tw[f, j0 : j0 + G]

    adjoint_stage(tw, n_c1, wn, emit)
    for c in outs:
        c.wait()


def first_body(
    prec, codes, up, dn, bulk_o, bulk_e, cor_o, w1, image1, n_inc0, n_inc1, n_cr, n_cc, mis_in,
    mis, adj,
    n_prev, n_next, n_p0, n_pn, n_c0, n_cn, n_m0, n_a0, n_a1, ta, tb, tw, osem,
):
    del mis_in
    even = parity() == 0
    cor_e = bulk_e.at[136:160]
    fill(prec.at[0], n_p0)
    own_codes(codes, 0, n_c0, up, dn, 0)
    for j in range(NJ):
        halo(n_p0, j, pltpu.roll(blk(up, 16, j), 5, 0), pltpu.roll(blk(dn, 16, j), 3, 0))

    def previous(bulk, cor):
        for j in range(NJ):
            for b in range(8):
                n_prev[j, 8 + 8 * b : 16 + 8 * b] = blk(bulk, 8 * b, j)
            halo(n_prev, j, blk(cor, 0, j), blk(cor, 8, j))

    def following(bulk, cor):
        for j in range(NJ):
            for b in range(8):
                n_next[j, 8 + 8 * b : 16 + 8 * b] = blk(bulk, 8 * b, j)
                n_pn[j, 8 + 8 * b : 16 + 8 * b] = blk(bulk, 64 + 8 * b, j)
                spread(n_cn, j, 8 + 8 * b, bulk[128 + b : 129 + b, j * L : (j + 1) * L])
            halo(n_next, j, blk(cor, 0, j), blk(cor, 8, j))
            spread(n_cn, j, 0, blk(cor, 0, j)[0:1])
            spread(n_cn, j, 72, blk(cor, 8, j)[7:8])
            halo(n_pn, j, pltpu.roll(blk(cor, 16, j), 5, 0), pltpu.roll(blk(cor, 16, j), 3, 0))

    @pl.when(even)
    def _():
        previous(bulk_o, cor_o)
        following(bulk_e, cor_e)

    @pl.when(jnp.logical_not(even))
    def _():
        previous(bulk_e, cor_e)
        following(bulk_o, cor_o)

    wn = (n_cr, n_cc)
    inside = inside_rows()
    misfit_stage(n_prev, n_inc0, n_c0, wn, ta, n_m0)
    outs = emit_out(n_m0, mis.at[0], osem, 0)
    smooth_stages(ta, tb, n_p0, tw, inside)
    for f in range(F):
        for j0 in range(0, NJ, G):
            save(n_a0, f, j0, tw[f, j0 : j0 + G] - image1[f, j0 : j0 + G])
    outs += emit_out(n_a0, adj.at[0], osem, NJ)
    misfit_stage(n_inc1, n_next, n_cn, wn, ta, None)
    smooth_stages(ta, tb, n_pn, tw, inside)
    adjoint_stage(
        tw, n_cn, wn, lambda f, j0, image: save(n_a1, f, j0, w1[f, j0 : j0 + G] - image)
    )
    outs += emit_out(n_a1, adj.at[1], osem, 2 * NJ)
    for c in outs:
        c.wait()


NAT = VMEM((NJ, 80, L), jnp.float32)
TFORM = VMEM((F, NJ, 8, L), jnp.float32)
ON_HBM = pl.BlockSpec(memory_space=pltpu.HBM)
ON_VMEM = pl.BlockSpec(memory_space=VMEM)
OUT = jax.ShapeDtypeStruct((2, 64, 2048), jnp.float32)


def last_step(*args):
    t = jax.ShapeDtypeStruct((F, NJ, 8, L), jnp.float32)
    n = jax.ShapeDtypeStruct((NJ, 80, L), jnp.float32)
    return pl.pallas_call(
        last_body,
        in_specs=[ON_VMEM] * 7,
        out_specs=[ON_HBM] + [ON_VMEM] * 6,
        out_shape=[OUT, t, t, n, n, n, n],
        scratch_shapes=[NAT] * 3 + [TFORM] * 3 + [pltpu.SemaphoreType.DMA((NJ,))],
        compiler_params=pltpu.CompilerParams(vmem_limit_bytes=24 << 20),
        name="last",
    )(*args)


def first_steps(*args):
    return pl.pallas_call(
        first_body,
        in_specs=[ON_VMEM] * 13 + [ON_HBM],
        out_specs=[ON_HBM] * 2,
        out_shape=[OUT, OUT],
        scratch_shapes=[NAT] * 9 + [TFORM] * 3 + [pltpu.SemaphoreType.DMA((3 * NJ,))],
        input_output_aliases={13: 0},
        compiler_params=pltpu.CompilerParams(vmem_limit_bytes=24 << 20),
        name="first",
    )(*args)


def permute(x, rule):
    axes = ("tm", "space")
    nt, ns = lax.axis_size("tm"), lax.axis_size("space")
    pairs = []
    for t in range(nt):
        for s in range(ns):
            a, b = rule(t, s)
            if 0 <= a < nt and 0 <= b < ns:
                pairs.append((t * ns + s, a * ns + b))
    return lax.ppermute(x, axes, pairs)


def off_chip(t, s):
    return (t - 1 if t % 2 == 0 else t + 1), s


def on_chip(t, s):
    return (t + 1 if t % 2 == 0 else t - 1), s


def up_on_even(t, s):
    return t, s + 1


def down_on_even(t, s):
    return t, s - 1


def on_device(inc, prec, cr, cc, codes):
    bulk_o, bulk_e, pass_1, pass_2 = pack(inc, prec, cr, cc, codes)
    bulk_o = permute(bulk_o, off_chip)
    pass_1 = permute(pass_1, up_on_even)
    pass_2 = permute(pass_2, down_on_even)
    up, dn, cor_o, bulk_e = corner(pass_1, pass_2, bulk_e)
    cor_o = permute(cor_o, off_chip)
    bulk_e = permute(bulk_e, on_chip)
    mis, *kept = last_step(inc, prec, cr, cc, codes, up, dn)
    return tuple(first_steps(prec, codes, up, dn, bulk_o, bulk_e, cor_o, *kept, mis))


def solution(mesh):
    in_specs = (
        P("tm", "space", None),
        P("tm", "space", None),
        P("space", None),
        P("space", None),
        P("tm", "space", None),
    )
    out_specs = (P("tm", "space", None), P("tm", "space", None))
    return jax.shard_map(
        on_device, mesh=mesh, in_specs=in_specs, out_specs=out_specs, check_vma=False
    )
```

```python
import jax
import jax.numpy as jnp
from jax import lax
from jax.experimental import pallas as pl
from jax.experimental.pallas import tpu as pltpu
from jax.sharding import PartitionSpec as P


F = 10
NJ = 16
G = 4
L = 128
C4 = 0.04 * 0.04
VMEM = pltpu.VMEM


def lanes():
    return lax.broadcasted_iota(jnp.int32, (1, 8, L), 2)


def sublanes(shape):
    return lax.broadcasted_iota(jnp.int32, shape, len(shape) - 2)


def load(nat, f, j0, n):
    return jnp.stack([nat[(j0 + g) % NJ, pl.ds(f, 8, stride=F), :] for g in range(n)])


def save(nat, f, j0, x):
    for g in range(G):
        nat[j0 + g, pl.ds(f, 8, stride=F), :] = x[g]


def load_t(t, f, j0, n):
    parts = []
    if j0 < 0:
        parts.append(t[f, NJ - 1 : NJ])
    parts.append(t[f, max(j0, 0) : min(j0 + n, NJ)])
    if j0 + n > NJ:
        parts.append(t[f, 0:1])
    return parts[0] if len(parts) == 1 else jnp.concatenate(parts, axis=0)


def masks(code):
    mc = code < 1.5
    mr = jnp.where(mc, code, code - 2.0) < 0.5
    return mr, mc


def stencil(get, visit):
    first = lanes() == 0
    last = lanes() == L - 1
    for f in range(F):
        before = pltpu.roll(get(f, NJ - 1, 1), 1, 2)
        here = get(f, 0, G)
        back = pltpu.roll(here, L - 1, 2)
        start = back[:1]
        for j0 in range(0, NJ, G):
            if j0 + G < NJ:
                there = get(f, j0 + G, G)
                back_there = pltpu.roll(there, L - 1, 2)
                edge = back_there[:1]
            else:
                there = back_there = None
                edge = start
            fore = pltpu.roll(here, 1, 2)
            left = jnp.where(first, jnp.concatenate([before, fore[: G - 1]], axis=0), fore)
            right = jnp.where(last, jnp.concatenate([back[1:], edge], axis=0), back)
            above = get(f - 1, j0, G) if f > 0 else pltpu.roll(get(F - 1, j0, G), 1, 1)
            below = get(f + 1, j0, G) if f < F - 1 else pltpu.roll(get(0, j0, G), 7, 1)
            visit(f, j0, here, left, right, above, below)
            before = fore[G - 1 :]
            here, back = there, back_there


def misfit_stage(un, vn, code, wn, tout, out):
    def visit(f, j0, u, left, right, up, down):
        mr, mc = masks(load(code, f, j0, G))
        cr, cc = load(wn[0], f, j0, G), load(wn[1], f, j0, G)
        moved = (
            (1.0 - cr - cc) * u
            + cr * jnp.where(mr, up, down)
            + cc * jnp.where(mc, left, right)
        )
        mis = load(vn, f, j0, G) - moved
        tout[f, j0 : j0 + G] = mis
        if out is not None:
            save(out, f, j0, mis)

    stencil(lambda f, j0, n: load(un, f, j0, n), visit)


def sweep_stage(tin, tout, after):
    def visit(f, j0, u, left, right, up, down):
        x = ((up + down) + (left + right)) + u
        tout[f, j0 : j0 + G] = after(x, f, j0)

    stencil(lambda f, j0, n: load_t(tin, f, j0, n), visit)


def smooth_stages(tin, tmp, pn, tout, inside):
    def mask(x, f, j0):
        return jnp.where(inside(f), x, 0.0)

    def scale(x, f, j0):
        return (load(pn, f, j0, G) * C4) * x

    sweep_stage(tin, tmp, mask)
    sweep_stage(tmp, tin, scale)
    sweep_stage(tin, tmp, mask)
    sweep_stage(tmp, tout, lambda x, f, j0: x)


def adjoint_stage(tw, code, wn, emit, done=lambda j0: None):
    first = lanes() == 0
    last = lanes() == L - 1

    def pieces(f, j0):
        w = load_t(tw, f, j0 - 1, G + 2)
        mr, mc = masks(load(code, f, j0 - 1, G + 2))
        mr = mr[1 : G + 1]
        cr = load(wn[0], f, j0, G)
        cc = load(wn[1], f, j0 - 1, G + 2)
        mid = w[1 : G + 1]
        rows = cr * mid
        lower = jnp.where(mr, rows, 0.0)
        cols = cc * w
        plus = pltpu.roll(jnp.where(mc, cols, 0.0)[1:], L - 1, 2)
        minus = pltpu.roll(jnp.where(mc, 0.0, cols)[: G + 1], 1, 2)
        image = (
            (1.0 - cr - cc[1 : G + 1]) * mid
            + jnp.where(last, plus[1:], plus[:G])
            + jnp.where(first, minus[:G], minus[1:])
        )
        return image, lower, rows - lower

    def upper_only(f, j0):
        mr, _ = masks(load(code, f, j0, G))
        return jnp.where(mr, 0.0, load(wn[0], f, j0, G) * load_t(tw, f, j0, G))

    for j0 in range(0, NJ, G):
        above = pltpu.roll(upper_only(F - 1, j0), 1, 1)
        image, lower, upper = pieces(0, j0)
        lower0 = pltpu.roll(lower, 7, 1)
        for f in range(F):
            if f < F - 1:
                after = pieces(f + 1, j0)
                below = after[1]
            else:
                after = None
                below = lower0
            emit(f, j0, image + (above + below))
            above = upper
            if after is not None:
                image, lower, upper = after
        done(j0)


def parity():
    return lax.axis_index("tm") % 2


def code_rows(codes, step):
    c = codes[step].astype(jnp.float32)
    return [jnp.broadcast_to(c[:, j : j + 1], (8, L)) for j in range(NJ)]


def pack_kernel(copies, inc, prec, edge, codes, bulk_o, bulk_e, pass_1, pass_2, sems):
    even = parity() == 0

    def forward(dst):
        return [pltpu.make_async_copy(inc.at[1], dst.at[pl.ds(0, 64)], sems.at[0])]

    def backward(dst):
        return [
            pltpu.make_async_copy(inc.at[0], dst.at[pl.ds(0, 64)], sems.at[1]),
            pltpu.make_async_copy(prec.at[0], dst.at[pl.ds(64, 64)], sems.at[2]),
        ]

    def start(fwd, bwd):
        for c in forward(fwd) + backward(bwd):
            c.start()

    @pl.when(even)
    def _():
        start(bulk_e, bulk_o)

    @pl.when(jnp.logical_not(even))
    def _():
        start(bulk_o, bulk_e)

    for c in copies:
        c.wait()
    row = sublanes((8, L))
    rows0 = code_rows(codes, 0)
    rows1 = code_rows(codes, 1)
    for j in range(NJ):
        cols = pl.ds(j * L, L)
        bulk_o[128:136, cols] = rows0[j]
        bulk_e[128:136, cols] = rows0[j]

    def edges(up, dn):
        for j in range(NJ):
            cols = pl.ds(j * L, L)
            inc0t, inc0b, inc1t, inc1b, p0t, p0b, p1t, p1b, crt, crb, cct, ccb = [
                edge[k, :, cols] for k in range(12)
            ]
            c0t = jnp.broadcast_to(rows0[j][0:1], (8, L))
            c0b = jnp.broadcast_to(rows0[j][7:8], (8, L))
            c1t = jnp.broadcast_to(rows1[j][0:1], (8, L))
            c1b = jnp.broadcast_to(rows1[j][7:8], (8, L))
            up[0:8, cols] = jnp.where(row < 2, c0b, inc0b)
            up[8:16, cols] = jnp.where(row < 2, c1b, inc1b)
            up[16:24, cols] = jnp.where(row < 3, pltpu.roll(p0b, 3, 0), crb)
            up[24:32, cols] = jnp.where(row < 3, pltpu.roll(p1b, 3, 0), ccb)
            dn[0:8, cols] = jnp.where(row > 5, c0t, inc0t)
            dn[8:16, cols] = jnp.where(row > 5, c1t, inc1t)
            dn[16:24, cols] = jnp.where(row > 4, pltpu.roll(p0t, 5, 0), crt)
            dn[24:32, cols] = jnp.where(row > 4, pltpu.roll(p1t, 5, 0), cct)

    edges(pass_1, pass_2)

    @pl.when(even)
    def _():
        for c in forward(bulk_e) + backward(bulk_o):
            c.wait()

    @pl.when(jnp.logical_not(even))
    def _():
        for c in forward(bulk_o) + backward(bulk_e):
            c.wait()


def pack_body(inc, prec, cr, cc, codes_hbm, bulk_o, bulk_e, pass_1, pass_2, codes, edge, sems, esems):
    top, bottom = pl.ds(0, 8), pl.ds(56, 8)
    srcs = []
    for a in (inc.at[0], inc.at[1], prec.at[0], prec.at[1], cr, cc):
        srcs += [a.at[top], a.at[bottom]]
    copies = [pltpu.make_async_copy(codes_hbm, codes, esems.at[12])]
    copies += [pltpu.make_async_copy(s, edge.at[k], esems.at[k]) for k, s in enumerate(srcs)]
    for c in copies:
        c.start()
    pack_kernel(copies, inc, prec, edge, codes, bulk_o, bulk_e, pass_1, pass_2, sems)


def pack(inc, prec, cr, cc, codes):
    any_spec = pl.BlockSpec(memory_space=pltpu.HBM)
    vmem = pl.BlockSpec(memory_space=VMEM)
    f32 = lambda *s: jax.ShapeDtypeStruct(s, jnp.float32)
    return pl.pallas_call(
        pack_body,
        in_specs=[any_spec] * 5,
        out_specs=[vmem] * 4,
        out_shape=[f32(136, 2048), f32(160, 2048), f32(32, 2048), f32(32, 2048)],
        scratch_shapes=[
            VMEM((2, 8, 16), jnp.int32),
            VMEM((12, 8, 2048), jnp.float32),
            pltpu.SemaphoreType.DMA((3,)),
            pltpu.SemaphoreType.DMA((13,)),
        ],
        compiler_params=pltpu.CompilerParams(vmem_limit_bytes=12 << 20),
        name="pack",
    )(*(pltpu.with_memory_space_constraint(a, pltpu.HBM) for a in (inc, prec, cr, cc, codes)))


def corner_body(pass_1, pass_2, bulk_in, up, dn, cor_o, bulk_e):
    del bulk_in
    cor_e = bulk_e.at[136:160]
    even = parity() == 0
    row = sublanes((8, 2048))

    def forward(up, dn, dst):
        dst[0:8, :] = up[8:16, :]
        dst[8:16, :] = dn[8:16, :]
        dst[16:24, :] = up[8:16, :]

    def backward(up, dn, dst):
        dst[0:8, :] = up[0:8, :]
        dst[8:16, :] = dn[0:8, :]
        dst[16:24, :] = jnp.where(row < 4, up[16:24, :], dn[16:24, :])

    def both(from_up, from_dn, fwd, bwd):
        up[...] = from_up[...]
        dn[...] = from_dn[...]
        forward(from_up, from_dn, fwd)
        backward(from_up, from_dn, bwd)

    @pl.when(even)
    def _():
        both(pass_1, pass_2, cor_e, cor_o)

    @pl.when(jnp.logical_not(even))
    def _():
        both(pass_1, pass_2, cor_o, cor_e)


def corner(pass_1, pass_2, bulk_e):
    vmem = pl.BlockSpec(memory_space=VMEM)
    f32 = lambda *s: jax.ShapeDtypeStruct(s, jnp.float32)
    return pl.pallas_call(
        corner_body,
        in_specs=[vmem] * 2 + [pl.BlockSpec(memory_space=pl.ANY)],
        out_specs=[vmem] * 4,
        out_shape=[f32(32, 2048), f32(32, 2048), f32(24, 2048), f32(160, 2048)],
        input_output_aliases={2: 3},
        compiler_params=pltpu.CompilerParams(vmem_limit_bytes=8 << 20),
        name="corner",
    )(pass_1, pass_2, bulk_e)


def blk(ref, r, j):
    return ref[r : r + 8, j * L : (j + 1) * L]


def spread(dst, j, at, x):
    dst[j, at : at + 8] = jnp.broadcast_to(x, (8, L))


def halo(dst, j, top, bottom):
    dst[j, 0:8] = top
    dst[j, 72:80] = bottom


def fill(src, dst):
    for j in range(NJ):
        for b in range(8):
            dst[j, 8 + 8 * b : 16 + 8 * b] = src[8 * b : 8 * b + 8, j * L : (j + 1) * L]


def emit_out(nat, dst, sem, base, blocks=range(NJ)):
    copies = [
        pltpu.make_async_copy(
            nat.at[j, pl.ds(8, 64)], dst.at[:, pl.ds(j * L, L)], sem.at[base + j]
        )
        for j in blocks
    ]
    for c in copies:
        c.start()
    return copies


def inside_rows():
    slab = lax.axis_index("space")
    sub = sublanes((1, 8, L))
    top_out = (sub == 0) & (slab == 0)
    bottom_out = (sub == 7) & (slab == lax.axis_size("space") - 1)

    def inside(f):
        bad = None
        if f < 8:
            bad = top_out
        if f >= 2:
            bad = bottom_out if bad is None else bad | bottom_out
        return jnp.logical_not(bad)

    return inside


def own_codes(codes, step, n_c):
    rows = code_rows(codes, step)
    for j in range(NJ):
        for b in range(8):
            spread(n_c, j, 8 + 8 * b, rows[j][b : b + 1])


def halo_codes(n_c, up, dn, r):
    for j in range(NJ):
        spread(n_c, j, 0, blk(up, r, j)[0:1])
        spread(n_c, j, 72, blk(dn, r, j)[7:8])


def prepare_body(
    inc, prec, cr, cc, codes, n_inc0, n_inc1, n_cr, n_cc, n_p0, n_p1, n_c0, n_c1
):
    for src, dst in (
        (inc.at[0], n_inc0), (inc.at[1], n_inc1), (cr, n_cr), (cc, n_cc),
        (prec.at[0], n_p0), (prec.at[1], n_p1),
    ):
        fill(src, dst)
    own_codes(codes, 0, n_c0)
    own_codes(codes, 1, n_c1)


def last_body(
    up, dn, in_inc0, in_inc1, in_cr, in_cc, in_p1, in_c1,
    mis, w_out, image_out, n_inc0, n_inc1, n_cr, n_cc, n_p1, n_c1,
    n_m1, ta, tb, tw, osem,
):
    del in_inc0, in_inc1, in_cr, in_cc, in_p1, in_c1
    halo_codes(n_c1, up, dn, 8)
    for j in range(NJ):
        halo(n_inc0, j, blk(up, 0, j), blk(dn, 0, j))
        halo(n_inc1, j, blk(up, 8, j), blk(dn, 8, j))
        halo(n_cr, j, blk(up, 16, j), blk(dn, 16, j))
        halo(n_cc, j, blk(up, 24, j), blk(dn, 24, j))
        halo(n_p1, j, pltpu.roll(blk(up, 24, j), 5, 0), pltpu.roll(blk(dn, 24, j), 3, 0))
    wn = (n_cr, n_cc)
    inside = inside_rows()
    misfit_stage(n_inc0, n_inc1, n_c1, wn, ta, n_m1)
    outs = emit_out(n_m1, mis.at[1], osem, 0)
    smooth_stages(ta, tb, n_p1, tw, inside)

    def emit(f, j0, image):
        image_out[f, j0 : j0 + G] = image
        w_out[f, j0 : j0 + G] = tw[f, j0 : j0 + G]

    adjoint_stage(tw, n_c1, wn, emit)
    for c in outs:
        c.wait()


def first_body(
    up, dn, bulk_o, bulk_e, cor_o, w1, image1, n_inc0, n_inc1, n_cr, n_cc, in_p0, in_c0, mis_in,
    mis, adj, n_p0, n_c0,
    n_prev, n_next, n_pn, n_cn, n_m0, n_a0, n_a1, ta, tb, tw, osem,
):
    del in_p0, in_c0, mis_in
    even = parity() == 0
    cor_e = bulk_e.at[136:160]
    halo_codes(n_c0, up, dn, 0)
    for j in range(NJ):
        halo(n_p0, j, pltpu.roll(blk(up, 16, j), 5, 0), pltpu.roll(blk(dn, 16, j), 3, 0))

    def previous(bulk, cor):
        for j in range(NJ):
            for b in range(8):
                n_prev[j, 8 + 8 * b : 16 + 8 * b] = blk(bulk, 8 * b, j)
            halo(n_prev, j, blk(cor, 0, j), blk(cor, 8, j))

    def following(bulk, cor):
        for j in range(NJ):
            for b in range(8):
                n_next[j, 8 + 8 * b : 16 + 8 * b] = blk(bulk, 8 * b, j)
                n_pn[j, 8 + 8 * b : 16 + 8 * b] = blk(bulk, 64 + 8 * b, j)
                spread(n_cn, j, 8 + 8 * b, bulk[128 + b : 129 + b, j * L : (j + 1) * L])
            halo(n_next, j, blk(cor, 0, j), blk(cor, 8, j))
            spread(n_cn, j, 0, blk(cor, 0, j)[0:1])
            spread(n_cn, j, 72, blk(cor, 8, j)[7:8])
            halo(n_pn, j, pltpu.roll(blk(cor, 16, j), 5, 0), pltpu.roll(blk(cor, 16, j), 3, 0))

    @pl.when(even)
    def _():
        previous(bulk_o, cor_o)
        following(bulk_e, cor_e)

    @pl.when(jnp.logical_not(even))
    def _():
        previous(bulk_e, cor_e)
        following(bulk_o, cor_o)

    wn = (n_cr, n_cc)
    inside = inside_rows()
    misfit_stage(n_prev, n_inc0, n_c0, wn, ta, n_m0)
    outs = emit_out(n_m0, mis.at[0], osem, 0)
    smooth_stages(ta, tb, n_p0, tw, inside)
    for f in range(F):
        for j0 in range(0, NJ, G):
            save(n_a0, f, j0, tw[f, j0 : j0 + G] - image1[f, j0 : j0 + G])
    outs += emit_out(n_a0, adj.at[0], osem, NJ)
    misfit_stage(n_inc1, n_next, n_cn, wn, ta, None)
    smooth_stages(ta, tb, n_pn, tw, inside)
    adjoint_stage(
        tw,
        n_cn,
        wn,
        lambda f, j0, image: save(n_a1, f, j0, w1[f, j0 : j0 + G] - image),
        lambda j0: outs.extend(emit_out(n_a1, adj.at[1], osem, 2 * NJ, range(j0, j0 + G))),
    )
    for c in outs:
        c.wait()


NAT = VMEM((NJ, 80, L), jnp.float32)
TFORM = VMEM((F, NJ, 8, L), jnp.float32)
ON_HBM = pl.BlockSpec(memory_space=pltpu.HBM)
ON_VMEM = pl.BlockSpec(memory_space=VMEM)
OUT = jax.ShapeDtypeStruct((2, 64, 2048), jnp.float32)


NAT_OUT = jax.ShapeDtypeStruct((NJ, 80, L), jnp.float32)
T_OUT = jax.ShapeDtypeStruct((F, NJ, 8, L), jnp.float32)


def prepare(*args):
    return pl.pallas_call(
        prepare_body,
        in_specs=[ON_VMEM] * 5,
        out_specs=[ON_VMEM] * 8,
        out_shape=[NAT_OUT] * 8,
        compiler_params=pltpu.CompilerParams(vmem_limit_bytes=16 << 20),
        name="prepare",
    )(*args)


def last_step(*args):
    return pl.pallas_call(
        last_body,
        in_specs=[ON_VMEM] * 8,
        out_specs=[ON_HBM] + [ON_VMEM] * 8,
        out_shape=[OUT, T_OUT, T_OUT] + [NAT_OUT] * 6,
        scratch_shapes=[NAT] + [TFORM] * 3 + [pltpu.SemaphoreType.DMA((NJ,))],
        input_output_aliases={2 + k: 3 + k for k in range(6)},
        compiler_params=pltpu.CompilerParams(vmem_limit_bytes=24 << 20),
        name="last",
    )(*args)


def first_steps(*args):
    return pl.pallas_call(
        first_body,
        in_specs=[ON_VMEM] * 13 + [ON_HBM],
        out_specs=[ON_HBM] * 2 + [ON_VMEM] * 2,
        out_shape=[OUT, OUT, NAT_OUT, NAT_OUT],
        scratch_shapes=[NAT] * 7 + [TFORM] * 3 + [pltpu.SemaphoreType.DMA((3 * NJ,))],
        input_output_aliases={13: 0, 11: 2, 12: 3},
        compiler_params=pltpu.CompilerParams(vmem_limit_bytes=24 << 20),
        name="first",
    )(*args)


def permute(x, rule):
    axes = ("tm", "space")
    nt, ns = lax.axis_size("tm"), lax.axis_size("space")
    pairs = []
    for t in range(nt):
        for s in range(ns):
            a, b = rule(t, s)
            if 0 <= a < nt and 0 <= b < ns:
                pairs.append((t * ns + s, a * ns + b))
    return lax.ppermute(x, axes, pairs)


def off_chip(t, s):
    return (t - 1 if t % 2 == 0 else t + 1), s


def on_chip(t, s):
    return (t + 1 if t % 2 == 0 else t - 1), s


def up_on_even(t, s):
    return t, s + 1


def down_on_even(t, s):
    return t, s - 1


def on_device(inc, prec, cr, cc, codes):
    bulk_o, bulk_e, pass_1, pass_2 = pack(inc, prec, cr, cc, codes)
    bulk_o = permute(bulk_o, off_chip)
    pass_1 = permute(pass_1, up_on_even)
    pass_2 = permute(pass_2, down_on_even)
    up, dn, cor_o, bulk_e = corner(pass_1, pass_2, bulk_e)
    cor_o = permute(cor_o, off_chip)
    bulk_e = permute(bulk_e, on_chip)
    inc0, inc1, cr, cc, p0, p1, c0, c1 = prepare(inc, prec, cr, cc, codes)
    mis, w1, image1, inc0, inc1, cr, cc, _, _ = last_step(up, dn, inc0, inc1, cr, cc, p1, c1)
    outs = first_steps(up, dn, bulk_o, bulk_e, cor_o, w1, image1, inc0, inc1, cr, cc, p0, c0, mis)
    return outs[0], outs[1]


def solution(mesh):
    in_specs = (
        P("tm", "space", None),
        P("tm", "space", None),
        P("space", None),
        P("space", None),
        P("tm", "space", None),
    )
    out_specs = (P("tm", "space", None), P("tm", "space", None))
    return jax.shard_map(
        on_device, mesh=mesh, in_specs=in_specs, out_specs=out_specs, check_vma=False
    )
```

```python
import jax
import jax.numpy as jnp
from jax import lax
from jax.experimental import pallas as pl
from jax.experimental.pallas import tpu as pltpu
from jax.sharding import PartitionSpec as P


F = 10
NJ = 16
G = 4
L = 128
C4 = 0.04 * 0.04
VMEM = pltpu.VMEM


def lanes():
    return lax.broadcasted_iota(jnp.int32, (1, 8, L), 2)


def sublanes(shape):
    return lax.broadcasted_iota(jnp.int32, shape, len(shape) - 2)


def load(nat, f, j0, n):
    return jnp.stack([nat[(j0 + g) % NJ, pl.ds(f, 8, stride=F), :] for g in range(n)])


def save(nat, f, j0, x):
    for g in range(G):
        nat[j0 + g, pl.ds(f, 8, stride=F), :] = x[g]


def load_t(t, f, j0, n):
    parts = []
    if j0 < 0:
        parts.append(t[f, NJ - 1 : NJ])
    parts.append(t[f, max(j0, 0) : min(j0 + n, NJ)])
    if j0 + n > NJ:
        parts.append(t[f, 0:1])
    return parts[0] if len(parts) == 1 else jnp.concatenate(parts, axis=0)


def masks(code):
    mc = code < 1.5
    mr = jnp.where(mc, code, code - 2.0) < 0.5
    return mr, mc


def stencil(get, visit):
    first = lanes() == 0
    last = lanes() == L - 1
    for f in range(F):
        before = pltpu.roll(get(f, NJ - 1, 1), 1, 2)
        here = get(f, 0, G)
        back = pltpu.roll(here, L - 1, 2)
        start = back[:1]
        for j0 in range(0, NJ, G):
            if j0 + G < NJ:
                there = get(f, j0 + G, G)
                back_there = pltpu.roll(there, L - 1, 2)
                edge = back_there[:1]
            else:
                there = back_there = None
                edge = start
            fore = pltpu.roll(here, 1, 2)
            left = jnp.where(first, jnp.concatenate([before, fore[: G - 1]], axis=0), fore)
            right = jnp.where(last, jnp.concatenate([back[1:], edge], axis=0), back)
            above = get(f - 1, j0, G) if f > 0 else pltpu.roll(get(F - 1, j0, G), 1, 1)
            below = get(f + 1, j0, G) if f < F - 1 else pltpu.roll(get(0, j0, G), 7, 1)
            visit(f, j0, here, left, right, above, below)
            before = fore[G - 1 :]
            here, back = there, back_there


def misfit_stage(un, vn, code, wn, tout, out):
    def visit(f, j0, u, left, right, up, down):
        mr, mc = masks(load(code, f, j0, G))
        cr, cc = load(wn[0], f, j0, G), load(wn[1], f, j0, G)
        moved = (
            (1.0 - cr - cc) * u
            + cr * jnp.where(mr, up, down)
            + cc * jnp.where(mc, left, right)
        )
        mis = load(vn, f, j0, G) - moved
        tout[f, j0 : j0 + G] = mis
        if out is not None:
            save(out, f, j0, mis)

    stencil(lambda f, j0, n: load(un, f, j0, n), visit)


def sweep_stage(tin, tout, after):
    def visit(f, j0, u, left, right, up, down):
        x = ((up + down) + (left + right)) + u
        tout[f, j0 : j0 + G] = after(x, f, j0)

    stencil(lambda f, j0, n: load_t(tin, f, j0, n), visit)


def smooth_stages(tin, tmp, pn, tout, inside):
    def mask(x, f, j0):
        return jnp.where(inside(f), x, 0.0)

    def scale(x, f, j0):
        return (load(pn, f, j0, G) * C4) * x

    sweep_stage(tin, tmp, mask)
    sweep_stage(tmp, tin, scale)
    sweep_stage(tin, tmp, mask)
    sweep_stage(tmp, tout, lambda x, f, j0: x)


def adjoint_stage(tw, code, wn, emit, done=lambda j0: None):
    first = lanes() == 0
    last = lanes() == L - 1

    def pieces(f, j0):
        w = load_t(tw, f, j0 - 1, G + 2)
        mr, mc = masks(load(code, f, j0 - 1, G + 2))
        mr = mr[1 : G + 1]
        cr = load(wn[0], f, j0, G)
        cc = load(wn[1], f, j0 - 1, G + 2)
        mid = w[1 : G + 1]
        rows = cr * mid
        lower = jnp.where(mr, rows, 0.0)
        cols = cc * w
        plus = pltpu.roll(jnp.where(mc, cols, 0.0)[1:], L - 1, 2)
        minus = pltpu.roll(jnp.where(mc, 0.0, cols)[: G + 1], 1, 2)
        image = (
            (1.0 - cr - cc[1 : G + 1]) * mid
            + jnp.where(last, plus[1:], plus[:G])
            + jnp.where(first, minus[:G], minus[1:])
        )
        return image, lower, rows - lower

    def upper_only(f, j0):
        mr, _ = masks(load(code, f, j0, G))
        return jnp.where(mr, 0.0, load(wn[0], f, j0, G) * load_t(tw, f, j0, G))

    for j0 in range(0, NJ, G):
        above = pltpu.roll(upper_only(F - 1, j0), 1, 1)
        image, lower, upper = pieces(0, j0)
        lower0 = pltpu.roll(lower, 7, 1)
        for f in range(F):
            if f < F - 1:
                after = pieces(f + 1, j0)
                below = after[1]
            else:
                after = None
                below = lower0
            emit(f, j0, image + (above + below))
            above = upper
            if after is not None:
                image, lower, upper = after
        done(j0)


def parity():
    return lax.axis_index("tm") % 2


def code_rows(codes, step):
    c = codes[step].astype(jnp.float32)
    return [jnp.broadcast_to(c[:, j : j + 1], (8, L)) for j in range(NJ)]


def pack_kernel(copies, inc, prec, edge, codes, bulk_o, bulk_e, pass_1, pass_2, sems):
    even = parity() == 0

    def forward(dst):
        return [pltpu.make_async_copy(inc.at[1], dst.at[pl.ds(0, 64)], sems.at[0])]

    def backward(dst):
        return [
            pltpu.make_async_copy(inc.at[0], dst.at[pl.ds(0, 64)], sems.at[1]),
            pltpu.make_async_copy(prec.at[0], dst.at[pl.ds(64, 64)], sems.at[2]),
        ]

    def start(fwd, bwd):
        for c in forward(fwd) + backward(bwd):
            c.start()

    @pl.when(even)
    def _():
        start(bulk_e, bulk_o)

    @pl.when(jnp.logical_not(even))
    def _():
        start(bulk_o, bulk_e)

    for c in copies:
        c.wait()
    row = sublanes((8, L))
    rows0 = code_rows(codes, 0)
    rows1 = code_rows(codes, 1)
    for j in range(NJ):
        cols = pl.ds(j * L, L)
        bulk_o[128:136, cols] = rows0[j]
        bulk_e[128:136, cols] = rows0[j]

    def edges(up, dn):
        for j in range(NJ):
            cols = pl.ds(j * L, L)
            inc0t, inc0b, inc1t, inc1b, p0t, p0b, p1t, p1b, crt, crb, cct, ccb = [
                edge[k, :, cols] for k in range(12)
            ]
            c0t = jnp.broadcast_to(rows0[j][0:1], (8, L))
            c0b = jnp.broadcast_to(rows0[j][7:8], (8, L))
            c1t = jnp.broadcast_to(rows1[j][0:1], (8, L))
            c1b = jnp.broadcast_to(rows1[j][7:8], (8, L))
            up[0:8, cols] = jnp.where(row < 2, c0b, inc0b)
            up[8:16, cols] = jnp.where(row < 2, c1b, inc1b)
            up[16:24, cols] = jnp.where(row < 3, pltpu.roll(p0b, 3, 0), crb)
            up[24:32, cols] = jnp.where(row < 3, pltpu.roll(p1b, 3, 0), ccb)
            dn[0:8, cols] = jnp.where(row > 5, c0t, inc0t)
            dn[8:16, cols] = jnp.where(row > 5, c1t, inc1t)
            dn[16:24, cols] = jnp.where(row > 4, pltpu.roll(p0t, 5, 0), crt)
            dn[24:32, cols] = jnp.where(row > 4, pltpu.roll(p1t, 5, 0), cct)

    edges(pass_1, pass_2)

    @pl.when(even)
    def _():
        for c in forward(bulk_e) + backward(bulk_o):
            c.wait()

    @pl.when(jnp.logical_not(even))
    def _():
        for c in forward(bulk_o) + backward(bulk_e):
            c.wait()


def pack_body(inc, prec, cr, cc, codes_hbm, bulk_o, bulk_e, pass_1, pass_2, codes, edge, sems, esems):
    top, bottom = pl.ds(0, 8), pl.ds(56, 8)
    srcs = []
    for a in (inc.at[0], inc.at[1], prec.at[0], prec.at[1], cr, cc):
        srcs += [a.at[top], a.at[bottom]]
    copies = [pltpu.make_async_copy(codes_hbm, codes, esems.at[12])]
    copies += [pltpu.make_async_copy(s, edge.at[k], esems.at[k]) for k, s in enumerate(srcs)]
    for c in copies:
        c.start()
    pack_kernel(copies, inc, prec, edge, codes, bulk_o, bulk_e, pass_1, pass_2, sems)


def pack(inc, prec, cr, cc, codes):
    any_spec = pl.BlockSpec(memory_space=pltpu.HBM)
    vmem = pl.BlockSpec(memory_space=VMEM)
    f32 = lambda *s: jax.ShapeDtypeStruct(s, jnp.float32)
    return pl.pallas_call(
        pack_body,
        in_specs=[any_spec] * 5,
        out_specs=[vmem] * 4,
        out_shape=[f32(136, 2048), f32(160, 2048), f32(32, 2048), f32(32, 2048)],
        scratch_shapes=[
            VMEM((2, 8, 16), jnp.int32),
            VMEM((12, 8, 2048), jnp.float32),
            pltpu.SemaphoreType.DMA((3,)),
            pltpu.SemaphoreType.DMA((13,)),
        ],
        compiler_params=pltpu.CompilerParams(vmem_limit_bytes=12 << 20),
        name="pack",
    )(*(pltpu.with_memory_space_constraint(a, pltpu.HBM) for a in (inc, prec, cr, cc, codes)))


def corner_body(up, dn, bulk_in, cor_o, bulk_e):
    del bulk_in
    cor_e = bulk_e.at[136:160]
    even = parity() == 0
    row = sublanes((8, 2048))

    def forward(up, dn, dst):
        dst[0:8, :] = up[8:16, :]
        dst[8:16, :] = dn[8:16, :]
        dst[16:24, :] = up[8:16, :]

    def backward(up, dn, dst):
        dst[0:8, :] = up[0:8, :]
        dst[8:16, :] = dn[0:8, :]
        dst[16:24, :] = jnp.where(row < 4, up[16:24, :], dn[16:24, :])

    def both(from_up, from_dn, fwd, bwd):
        forward(from_up, from_dn, fwd)
        backward(from_up, from_dn, bwd)

    @pl.when(even)
    def _():
        both(up, dn, cor_e, cor_o)

    @pl.when(jnp.logical_not(even))
    def _():
        both(up, dn, cor_o, cor_e)


def corner(pass_1, pass_2, bulk_e):
    vmem = pl.BlockSpec(memory_space=VMEM)
    f32 = lambda *s: jax.ShapeDtypeStruct(s, jnp.float32)
    return pl.pallas_call(
        corner_body,
        in_specs=[vmem] * 2 + [pl.BlockSpec(memory_space=pl.ANY)],
        out_specs=[vmem] * 2,
        out_shape=[f32(24, 2048), f32(160, 2048)],
        input_output_aliases={2: 1},
        compiler_params=pltpu.CompilerParams(vmem_limit_bytes=8 << 20),
        name="corner",
    )(pass_1, pass_2, bulk_e)


def blk(ref, r, j):
    return ref[r : r + 8, j * L : (j + 1) * L]


def spread(dst, j, at, x):
    dst[j, at : at + 8] = jnp.broadcast_to(x, (8, L))


def halo(dst, j, top, bottom):
    dst[j, 0:8] = top
    dst[j, 72:80] = bottom


def fill(src, dst):
    for j in range(NJ):
        for b in range(8):
            dst[j, 8 + 8 * b : 16 + 8 * b] = src[8 * b : 8 * b + 8, j * L : (j + 1) * L]


def emit_out(nat, dst, sem, base, blocks=range(NJ)):
    copies = [
        pltpu.make_async_copy(
            nat.at[j, pl.ds(8, 64)], dst.at[:, pl.ds(j * L, L)], sem.at[base + j]
        )
        for j in blocks
    ]
    for c in copies:
        c.start()
    return copies


def inside_rows():
    slab = lax.axis_index("space")
    sub = sublanes((1, 8, L))
    top_out = (sub == 0) & (slab == 0)
    bottom_out = (sub == 7) & (slab == lax.axis_size("space") - 1)

    def inside(f):
        bad = None
        if f < 8:
            bad = top_out
        if f >= 2:
            bad = bottom_out if bad is None else bad | bottom_out
        return jnp.logical_not(bad)

    return inside


def own_codes(codes, step, n_c):
    rows = code_rows(codes, step)
    for j in range(NJ):
        for b in range(8):
            spread(n_c, j, 8 + 8 * b, rows[j][b : b + 1])


def halo_codes(n_c, up, dn, r):
    for j in range(NJ):
        spread(n_c, j, 0, blk(up, r, j)[0:1])
        spread(n_c, j, 72, blk(dn, r, j)[7:8])


def prepare_body(
    inc, prec, cr, cc, codes, n_inc0, n_inc1, n_cr, n_cc, n_p0, n_p1, n_c0, n_c1
):
    for src, dst in (
        (inc.at[0], n_inc0), (inc.at[1], n_inc1), (cr, n_cr), (cc, n_cc),
        (prec.at[0], n_p0), (prec.at[1], n_p1),
    ):
        fill(src, dst)
    own_codes(codes, 0, n_c0)
    own_codes(codes, 1, n_c1)


def last_body(
    up, dn, in_inc0, in_inc1, in_cr, in_cc, in_p1, in_c1,
    mis, w_out, image_out, n_inc0, n_inc1, n_cr, n_cc, n_p1, n_c1,
    n_m1, ta, tb, tw, osem,
):
    del in_inc0, in_inc1, in_cr, in_cc, in_p1, in_c1
    halo_codes(n_c1, up, dn, 8)
    for j in range(NJ):
        halo(n_inc0, j, blk(up, 0, j), blk(dn, 0, j))
        halo(n_inc1, j, blk(up, 8, j), blk(dn, 8, j))
        halo(n_cr, j, blk(up, 16, j), blk(dn, 16, j))
        halo(n_cc, j, blk(up, 24, j), blk(dn, 24, j))
        halo(n_p1, j, pltpu.roll(blk(up, 24, j), 5, 0), pltpu.roll(blk(dn, 24, j), 3, 0))
    wn = (n_cr, n_cc)
    inside = inside_rows()
    misfit_stage(n_inc0, n_inc1, n_c1, wn, ta, n_m1)
    outs = emit_out(n_m1, mis.at[1], osem, 0)
    smooth_stages(ta, tb, n_p1, tw, inside)

    def emit(f, j0, image):
        image_out[f, j0 : j0 + G] = image
        w_out[f, j0 : j0 + G] = tw[f, j0 : j0 + G]

    adjoint_stage(tw, n_c1, wn, emit)
    for c in outs:
        c.wait()


def first_body(
    up, dn, bulk_o, bulk_e, cor_o, w1, image1, n_inc0, n_inc1, n_cr, n_cc, in_p0, in_c0, mis_in,
    mis, adj, n_p0, n_c0,
    n_prev, n_next, n_pn, n_cn, n_m0, n_a0, n_a1, ta, tb, tw, osem,
):
    del in_p0, in_c0, mis_in
    even = parity() == 0
    cor_e = bulk_e.at[136:160]
    halo_codes(n_c0, up, dn, 0)
    for j in range(NJ):
        halo(n_p0, j, pltpu.roll(blk(up, 16, j), 5, 0), pltpu.roll(blk(dn, 16, j), 3, 0))

    def previous(bulk, cor):
        for j in range(NJ):
            for b in range(8):
                n_prev[j, 8 + 8 * b : 16 + 8 * b] = blk(bulk, 8 * b, j)
            halo(n_prev, j, blk(cor, 0, j), blk(cor, 8, j))

    def following(bulk, cor):
        for j in range(NJ):
            for b in range(8):
                n_next[j, 8 + 8 * b : 16 + 8 * b] = blk(bulk, 8 * b, j)
                n_pn[j, 8 + 8 * b : 16 + 8 * b] = blk(bulk, 64 + 8 * b, j)
                spread(n_cn, j, 8 + 8 * b, bulk[128 + b : 129 + b, j * L : (j + 1) * L])
            halo(n_next, j, blk(cor, 0, j), blk(cor, 8, j))
            spread(n_cn, j, 0, blk(cor, 0, j)[0:1])
            spread(n_cn, j, 72, blk(cor, 8, j)[7:8])
            halo(n_pn, j, pltpu.roll(blk(cor, 16, j), 5, 0), pltpu.roll(blk(cor, 16, j), 3, 0))

    @pl.when(even)
    def _():
        previous(bulk_o, cor_o)
        following(bulk_e, cor_e)

    @pl.when(jnp.logical_not(even))
    def _():
        previous(bulk_e, cor_e)
        following(bulk_o, cor_o)

    wn = (n_cr, n_cc)
    inside = inside_rows()
    misfit_stage(n_prev, n_inc0, n_c0, wn, ta, n_m0)
    outs = emit_out(n_m0, mis.at[0], osem, 0)
    smooth_stages(ta, tb, n_p0, tw, inside)
    for f in range(F):
        for j0 in range(0, NJ, G):
            save(n_a0, f, j0, tw[f, j0 : j0 + G] - image1[f, j0 : j0 + G])
    outs += emit_out(n_a0, adj.at[0], osem, NJ)
    misfit_stage(n_inc1, n_next, n_cn, wn, ta, None)
    smooth_stages(ta, tb, n_pn, tw, inside)
    adjoint_stage(
        tw,
        n_cn,
        wn,
        lambda f, j0, image: save(n_a1, f, j0, w1[f, j0 : j0 + G] - image),
        lambda j0: outs.extend(emit_out(n_a1, adj.at[1], osem, 2 * NJ, range(j0, j0 + G))),
    )
    for c in outs:
        c.wait()


NAT = VMEM((NJ, 80, L), jnp.float32)
TFORM = VMEM((F, NJ, 8, L), jnp.float32)
ON_HBM = pl.BlockSpec(memory_space=pltpu.HBM)
ON_VMEM = pl.BlockSpec(memory_space=VMEM)
OUT = jax.ShapeDtypeStruct((2, 64, 2048), jnp.float32)


NAT_OUT = jax.ShapeDtypeStruct((NJ, 80, L), jnp.float32)
T_OUT = jax.ShapeDtypeStruct((F, NJ, 8, L), jnp.float32)


def prepare(*args):
    return pl.pallas_call(
        prepare_body,
        in_specs=[ON_VMEM] * 5,
        out_specs=[ON_VMEM] * 8,
        out_shape=[NAT_OUT] * 8,
        compiler_params=pltpu.CompilerParams(vmem_limit_bytes=16 << 20),
        name="prepare",
    )(*args)


def last_step(*args):
    return pl.pallas_call(
        last_body,
        in_specs=[ON_VMEM] * 8,
        out_specs=[ON_HBM] + [ON_VMEM] * 8,
        out_shape=[OUT, T_OUT, T_OUT] + [NAT_OUT] * 6,
        scratch_shapes=[NAT] + [TFORM] * 3 + [pltpu.SemaphoreType.DMA((NJ,))],
        input_output_aliases={2 + k: 3 + k for k in range(6)},
        compiler_params=pltpu.CompilerParams(vmem_limit_bytes=24 << 20),
        name="last",
    )(*args)


def first_steps(*args):
    return pl.pallas_call(
        first_body,
        in_specs=[ON_VMEM] * 13 + [ON_HBM],
        out_specs=[ON_HBM] * 2 + [ON_VMEM] * 2,
        out_shape=[OUT, OUT, NAT_OUT, NAT_OUT],
        scratch_shapes=[NAT] * 7 + [TFORM] * 3 + [pltpu.SemaphoreType.DMA((3 * NJ,))],
        input_output_aliases={13: 0, 11: 2, 12: 3},
        compiler_params=pltpu.CompilerParams(vmem_limit_bytes=24 << 20),
        name="first",
    )(*args)


def permute(x, rule):
    axes = ("tm", "space")
    nt, ns = lax.axis_size("tm"), lax.axis_size("space")
    pairs = []
    for t in range(nt):
        for s in range(ns):
            a, b = rule(t, s)
            if 0 <= a < nt and 0 <= b < ns:
                pairs.append((t * ns + s, a * ns + b))
    return lax.ppermute(x, axes, pairs)


def off_chip(t, s):
    return (t - 1 if t % 2 == 0 else t + 1), s


def on_chip(t, s):
    return (t + 1 if t % 2 == 0 else t - 1), s


def up_on_even(t, s):
    return t, s + 1


def down_on_even(t, s):
    return t, s - 1


def on_device(inc, prec, cr, cc, codes):
    bulk_o, bulk_e, pass_1, pass_2 = pack(inc, prec, cr, cc, codes)
    bulk_o = permute(bulk_o, off_chip)
    pass_1 = permute(pass_1, up_on_even)
    pass_2 = permute(pass_2, down_on_even)
    up, dn = pass_1, pass_2
    cor_o, bulk_e = corner(up, dn, bulk_e)
    cor_o = permute(cor_o, off_chip)
    bulk_e = permute(bulk_e, on_chip)
    inc0, inc1, cr, cc, p0, p1, c0, c1 = prepare(inc, prec, cr, cc, codes)
    mis, w1, image1, inc0, inc1, cr, cc, _, _ = last_step(up, dn, inc0, inc1, cr, cc, p1, c1)
    outs = first_steps(up, dn, bulk_o, bulk_e, cor_o, w1, image1, inc0, inc1, cr, cc, p0, c0, mis)
    return outs[0], outs[1]


def solution(mesh):
    in_specs = (
        P("tm", "space", None),
        P("tm", "space", None),
        P("space", None),
        P("space", None),
        P("tm", "space", None),
    )
    out_specs = (P("tm", "space", None), P("tm", "space", None))
    return jax.shard_map(
        on_device, mesh=mesh, in_specs=in_specs, out_specs=out_specs, check_vma=False
    )
```
